128 devices in a mesh: gx: 4 (over z), gy: 32 (over x, y, core).
Axes of the slice: x: 4, y: 4, z: 4, core: 2. Of those that a mesh axis runs over, the one named last changes fastest.
Arguments:
- grid_state: bfloat16 [32768, 1024], P(('gx', 'gy')), may hold values from -6 to 6
- mesh_state: bfloat16 [32768, 1024], P(('gx', 'gy')), may hold values from -6 to 6
- encode_block: int32 [32768], P(('gx', 'gy')), may hold values from 0 to 255, as said below
- neighbour_block: int32 [256], P(('gx', 'gy')), may hold values from 0 to 255, as said below
- decode_block: int32 [32768], P(('gx', 'gy')), may hold values from 0 to 255, as said below
- encode_grid_gain: float32 [1024], replicated, may hold values from 0.25 to 1.75
- encode_mesh_gain: float32 [1024], replicated, may hold values from 0.25 to 1.75
- process_gain: float32 [1024], replicated, may hold values from 0.25 to 1.75
- decode_grid_gain: float32 [1024], replicated, may hold values from 0.25 to 1.75
- decode_mesh_gain: float32 [1024], replicated, may hold values from 0.25 to 1.75
- encode_query: bfloat16 [1024, 1024], replicated, may hold values from -0.1875 to 0.1875
- encode_keyval: bfloat16 [1024, 2048], replicated, may hold values from -0.1875 to 0.1875
- encode_out: bfloat16 [1024, 1024], replicated, may hold values from -0.1875 to 0.1875
- process_qkv: bfloat16 [1024, 3072], replicated, may hold values from -0.1875 to 0.1875
- process_out: bfloat16 [1024, 1024], replicated, may hold values from -0.1875 to 0.1875
- decode_query: bfloat16 [1024, 1024], replicated, may hold values from -0.1875 to 0.1875
- decode_keyval: bfloat16 [1024, 2048], replicated, may hold values from -0.1875 to 0.1875
- decode_out: bfloat16 [1024, 1024], replicated, may hold values from -0.1875 to 0.1875
Outputs:
- grid_update: bfloat16 [32768, 1024], P(('gx', 'gy'))
The draws below stay inside these ranges and needn't reach their ends.
Inputs may be any that keep to these rules, and one draw needn't show every extreme that they name: `encode_block`: block b lies on the b // 2-th device of the order of mesh nodes. The grid points of one device name the blocks of one device at most 4 times in all; every block is named by some grid point; in every draw some device's blocks are named exactly 4 times by the grid points of every device. `neighbour_block`: never b itself, and at most two blocks away from b. `decode_block`: block b lies on the b // 2-th device. The grid points of one device name the blocks of one device at most 4 times in all; every block is named; in every draw some device's blocks are named exactly 4 times by the grid points of every device.
All inputs are finite; a program needn't handle non-finite values.
Results may differ from the reference program's by a relative error of at most 0.015.
Values may be sent and summed in bfloat16 or wider, within the bound.
A program may use at most 128 MiB of HBM per device.

```python
import jax
import jax.numpy as jnp
from jax import lax

D = 1024
HEADS = 16
BLOCK = 128
GRID_DEV = 256
MESH_DEV = 256
CAP = 4
GRID = 32768
MESH = 32768
N_GX = 4
N_GY = 32


def routed_blocks(key):
    devices = N_GX * N_GY
    per_device = MESH_DEV // BLOCK
    total_slots = devices * CAP
    hottest = jax.random.randint(jax.random.fold_in(key, 1), (), 0, devices)
    slot_owner = jnp.arange(total_slots, dtype=jnp.int32) // CAP
    slot_rank = jnp.arange(total_slots, dtype=jnp.int32) % CAP

    def one_source(source):
        subkeys = jax.random.split(jax.random.fold_in(key, source + 7), 3)
        scores = jax.random.permutation(subkeys[0], total_slots).astype(jnp.int32)
        forced = (slot_owner == hottest) | (slot_owner == source) & (slot_rank < per_device)
        scores = scores + forced.astype(jnp.int32) * (2 * total_slots)
        chosen = lax.top_k(scores, GRID_DEV)[1]
        owners = chosen // CAP
        ranks = chosen % CAP
        pinned = (owners == source) & (ranks < per_device)
        spares = jax.random.randint(subkeys[1], (GRID_DEV,), 0, per_device)
        blocks = owners * per_device + jnp.where(pinned, ranks, spares)
        return blocks[jax.random.permutation(subkeys[2], GRID_DEV)]
    return jax.vmap(one_source)(jnp.arange(devices, dtype=jnp.int32)).reshape(-1).astype(jnp.int32)


def draw_encode_block(key, part):
    return routed_blocks(jax.random.fold_in(key, 11))


def draw_decode_block(key, part):
    return routed_blocks(jax.random.fold_in(key, 23))


def draw_neighbour_block(key, part):
    total_blocks = N_GX * N_GY * (MESH_DEV // BLOCK)
    blocks = jnp.arange(total_blocks, dtype=jnp.int32)
    picks = jax.random.randint(jax.random.fold_in(key, 37), (total_blocks,), 0, 4)
    offsets = jnp.where(picks < 2, picks - 2, picks - 1)
    target = blocks + offsets
    outside = (target < 0) | (target >= total_blocks)
    return jnp.where(outside, blocks - offsets, target).astype(jnp.int32)


def levels(own_key, extent, cuts, smallest, largest):
    level, own = 1.0, jax.random.fold_in(own_key, 6)
    for dim, parts in cuts:
        draws = jnp.exp(jax.random.uniform(jax.random.fold_in(own, dim), (parts,), jnp.float32, smallest / len(cuts), largest / len(cuts)))
        level = level * jnp.repeat(draws, extent[dim] // parts).reshape([-1 if axis == dim else 1 for axis in range(len(extent))])
    return level


def bell_draw(own_key, dims, width, limit, cuts=(), kind=jnp.bfloat16):
    factor_of = levels(own_key, dims, cuts, -0.22, 0.18) if cuts else 1.0
    values = jax.random.normal(own_key, dims, jnp.float32) * width * factor_of
    return jnp.minimum(jnp.maximum(values, -limit), limit).astype(kind)


def setup_inputs(seed: int = 0) -> dict:
    key_list = jax.random.split(jax.random.key(seed), 19)
    return {
        "grid_state": bell_draw(key_list[0], (GRID, D), 1.0, 6.0, ((0, 128),)),
        "mesh_state": bell_draw(key_list[1], (MESH, D), 1.0, 6.0, ((0, 128),)),
        "encode_block": draw_encode_block(jax.random.fold_in(key_list[18], 71), 0),
        "neighbour_block": draw_neighbour_block(jax.random.fold_in(key_list[18], 71), 0),
        "decode_block": draw_decode_block(jax.random.fold_in(key_list[18], 71), 0),
        "encode_grid_gain": jnp.clip(1.0 + 0.15 * jax.random.normal(key_list[5], (D,), jnp.float32), 0.25, 1.75),
        "encode_mesh_gain": jnp.clip(1.0 + 0.15 * jax.random.normal(key_list[6], (D,), jnp.float32), 0.25, 1.75),
        "process_gain": jnp.clip(1.0 + 0.15 * jax.random.normal(key_list[7], (D,), jnp.float32), 0.25, 1.75),
        "decode_grid_gain": jnp.clip(1.0 + 0.15 * jax.random.normal(key_list[8], (D,), jnp.float32), 0.25, 1.75),
        "decode_mesh_gain": jnp.clip(1.0 + 0.15 * jax.random.normal(key_list[9], (D,), jnp.float32), 0.25, 1.75),
        "encode_query": bell_draw(key_list[10], (D, D), D ** -0.5, 0.1875),
        "encode_keyval": bell_draw(key_list[11], (D, 2 * D), D ** -0.5, 0.1875),
        "encode_out": bell_draw(key_list[12], (D, D), D ** -0.5, 0.1875),
        "process_qkv": bell_draw(key_list[13], (D, 3 * D), D ** -0.5, 0.1875),
        "process_out": bell_draw(key_list[14], (D, D), D ** -0.5, 0.1875),
        "decode_query": bell_draw(key_list[15], (D, D), D ** -0.5, 0.1875),
        "decode_keyval": bell_draw(key_list[16], (D, 2 * D), D ** -0.5, 0.1875),
        "decode_out": bell_draw(key_list[17], (D, D), D ** -0.5, 0.1875),
    }


masked_score = -1e+30

def norm_rows(values, row_gain):
    wide = values.astype(jnp.float32)
    return wide * lax.rsqrt(lax.optimization_barrier(jnp.mean(wide * wide, axis=-1, keepdims=True)) + 1e-06) * row_gain

def attend(queries, keyval, allowed):
    features = queries.shape[-1]
    head_size = features // HEADS
    query_heads = queries.astype(jnp.float32).reshape(queries.shape[0], HEADS, head_size)
    key_heads = keyval[:, :features].astype(jnp.float32).reshape(keyval.shape[0], HEADS, head_size)
    value_heads = keyval[:, features:].astype(jnp.float32).reshape(keyval.shape[0], HEADS, head_size)
    scores = jnp.einsum('qhd,khd->hqk', query_heads, key_heads) * head_size ** (-0.5)
    scores = jnp.where(allowed[None], scores, masked_score)
    highest = lax.optimization_barrier(jnp.max(scores, axis=-1, keepdims=True))
    powers = jnp.exp(scores - highest)
    chances = (powers / lax.optimization_barrier(jnp.sum(powers, axis=-1, keepdims=True))).astype(jnp.bfloat16)
    output = jnp.einsum('hqk,khd->qhd', chances.astype(jnp.float32), value_heads)
    return output.reshape(queries.shape[0], features).astype(jnp.bfloat16)

def project(values, weight):
    return jnp.dot(values, weight, preferred_element_type=jnp.float32).astype(jnp.bfloat16)

def reference(grid_state, mesh_state, encode_block, neighbour_block, decode_block, encode_grid_gain, encode_mesh_gain, process_gain, decode_grid_gain, decode_mesh_gain, encode_query, encode_keyval, encode_out, process_qkv, process_out, decode_query, decode_keyval, decode_out):
    devices = N_GX * N_GY
    block_count = MESH_DEV // BLOCK
    slot_total = CAP * devices
    grid_count = grid_state.shape[0]
    features = grid_state.shape[1]
    blocks_all = mesh_state.shape[0] // BLOCK
    grid_keyval = project(norm_rows(grid_state, encode_grid_gain).astype(jnp.bfloat16), encode_keyval)
    mesh_query = project(norm_rows(mesh_state, encode_mesh_gain).astype(jnp.bfloat16), encode_query)
    owners = (encode_block // block_count).astype(jnp.int32)
    sorted_ids = jnp.argsort(owners, stable=True).astype(jnp.int32)
    counts = jnp.zeros((devices,), jnp.int32).at[owners].add(1)
    starts = (jnp.cumsum(counts) - counts).astype(jnp.int32)
    node_block = jnp.arange(MESH_DEV, dtype=jnp.int32) // BLOCK

    def encode(device):
        places = jnp.arange(slot_total, dtype=jnp.int32)
        filled = places < counts[device]
        row_ids = sorted_ids[jnp.minimum(starts[device] + places, grid_count - 1)]
        labels = jnp.where(filled, encode_block[row_ids] % block_count, -1).astype(jnp.int32)
        queries = lax.dynamic_slice_in_dim(mesh_query, (device * MESH_DEV).astype(jnp.int32), MESH_DEV, 0)
        return attend(queries, grid_keyval[row_ids], node_block[:, None] == labels[None, :])
    encoded = lax.map(encode, jnp.arange(devices, dtype=jnp.int32)).reshape(-1, features)
    mesh_mid = (mesh_state.astype(jnp.float32) + jnp.dot(encoded, encode_out, preferred_element_type=jnp.float32)).astype(jnp.bfloat16)
    mesh_qkv = project(norm_rows(mesh_mid, process_gain).astype(jnp.bfloat16), process_qkv)
    mesh_blocks = mesh_qkv.reshape(blocks_all, BLOCK, 3 * features)
    everywhere = jnp.ones((BLOCK, 2 * BLOCK), dtype=jnp.bool_)

    def process(index):
        own_rows = mesh_blocks[index]
        other_rows = mesh_blocks[neighbour_block[index]]
        key_rows = jnp.concatenate([own_rows[:, features:], other_rows[:, features:]], axis=0)
        return attend(own_rows[:, :features], key_rows, everywhere)
    processed = lax.map(process, jnp.arange(blocks_all, dtype=jnp.int32)).reshape(-1, features)
    mesh_out = (mesh_mid.astype(jnp.float32) + jnp.dot(processed, process_out, preferred_element_type=jnp.float32)).astype(jnp.bfloat16)
    grid_query = project(norm_rows(grid_state, decode_grid_gain).astype(jnp.bfloat16), decode_query)
    mesh_keyval = project(norm_rows(mesh_out, decode_mesh_gain).astype(jnp.bfloat16), decode_keyval).reshape(blocks_all, BLOCK, 2 * features)
    single_row = jnp.ones((1, BLOCK), dtype=jnp.bool_)

    def decode(start):
        queries = lax.dynamic_slice_in_dim(grid_query, start, BLOCK, 0)
        labels = lax.dynamic_slice_in_dim(decode_block, start, BLOCK, 0)
        key_rows = mesh_keyval[labels]
        return jax.vmap(lambda query_row, key_block: attend(query_row[None], key_block, single_row)[0])(queries, key_rows)
    decoded = lax.map(decode, jnp.arange(0, grid_count, BLOCK, dtype=jnp.int32)).reshape(-1, features)
    return jnp.dot(decoded, decode_out, preferred_element_type=jnp.float32).astype(jnp.bfloat16)
```

```python
import functools

import jax
import jax.numpy as jnp
from jax import lax
from jax.experimental import pallas as pl
from jax.experimental.pallas import tpu as pltpu
from jax.sharding import PartitionSpec as P

HEADS = 16
BLOCK = 128
CAP = 4
DEVICES = 128
D = 1024
ROWS = 256
SLOTS = DEVICES * CAP
PAIR = 128
MASKED = -1e30
MESH = pl.DeviceIdType.MESH
BF = jnp.bfloat16
F32 = jnp.float32


def coordinates():
    gy = lax.axis_index("gy")
    return lax.axis_index("gx"), gy // 8, lax.rem(gy // 2, 4), lax.rem(gy, 2)


def device_at(z, x, y, c):
    return lax.rem(z + 4, 4), lax.rem(x + 4, 4) * 8 + lax.rem(y + 4, 4) * 2 + lax.rem(c + 2, 2)


def peer(k, sign):
    z, x, y, c = coordinates()
    return device_at(
        z + sign * lax.rem(k // 16, 4),
        x + sign * lax.rem(k, 4),
        y + sign * lax.rem(k // 4, 4),
        c + sign * (k // 64),
    )


def iota(shape, dim):
    return lax.broadcasted_iota(jnp.int32, shape, dim)


def ones_where(condition, dtype=BF):
    return jnp.where(condition, 1.0, 0.0).astype(dtype)


def matmul(a, b):
    return jnp.dot(a, b, preferred_element_type=F32)


def matmul_nt(a, b):
    return lax.dot_general(a, b, (((1,), (1,)), ((), ())), preferred_element_type=F32)


def norm_into(src, src_row, dst, dst_row, gain_ref, rows=ROWS):
    def step(i, carry):
        wide = src[pl.ds(pl.multiple_of(src_row + i * 32, 32), 32), :].astype(F32)
        scale = lax.rsqrt(jnp.mean(wide * wide, axis=-1, keepdims=True) + 1e-6)
        dst[pl.ds(pl.multiple_of(dst_row + i * 32, 32), 32), :] = (
            wide * scale * gain_ref[...]
        ).astype(BF)
        return carry

    lax.fori_loop(0, rows // 32, step, 0)


def project(a_ref, w_ref, columns, first_column, epilogue, tile=512):
    def step(n, carry):
        at = pl.multiple_of(n * tile, tile)
        out = matmul(a_ref[...], w_ref[:, pl.ds(pl.multiple_of(first_column + at, tile), tile)])
        epilogue(pl.ds(at, tile), out)
        return carry

    lax.fori_loop(0, columns // tile, step, 0)


def slot_plan(blocks):
    z, x, y, c = coordinates()
    owner = blocks >> 1
    k = (
        (((owner >> 3) & 3) - x & 3)
        + 4 * (((owner >> 1) & 3) - y & 3)
        + 16 * ((owner >> 5) - z & 3)
        + 64 * ((owner & 1) - c & 1)
    )
    matches = ones_where(iota((DEVICES, ROWS), 0) == k)
    earlier = ones_where(iota((ROWS, ROWS), 0) < iota((ROWS, ROWS), 1))
    counts = matmul(matches, earlier)
    rank = jnp.sum(matches.astype(F32) * counts, axis=0, keepdims=True).astype(jnp.int32)
    return matches, rank, k * CAP + rank


def label_table(matches, rank, blocks, base):
    coded = jnp.where(iota((PAIR, ROWS), 0) == rank + base, (blocks & 1) + 1, 0)
    return matmul_nt(matches, coded.astype(F32).astype(BF))


def interleave():
    m = iota((256, 256), 0)
    return ones_where(iota((256, 256), 1) == 64 * ((m >> 2) & 3) + 4 * (m >> 4) + (m & 3))


def separate():
    n = iota((256, 256), 0)
    return ones_where(iota((256, 256), 1) == 16 * ((n >> 2) & 15) + 4 * (n >> 6) + (n & 3))


def store_slabs(dst, j, rows, mix):
    tall = jnp.concatenate([rows[:, 256 * q : 256 * q + 256] for q in range(4)], axis=0)
    dst[pl.ds(16 * j, 16)] = matmul(mix, tall).astype(BF).reshape(16, 16, 256)


def load_slabs(src, j, unmix):
    tall = matmul(unmix, src[pl.ds(16 * j, 16)].reshape(256, 256)).astype(BF)
    return jnp.concatenate([tall[64 * q : 64 * q + 64] for q in range(4)], axis=1)


def pack(rows_ref, slot, dst, mix):
    def step(j, carry):
        chosen = ones_where(iota((64, ROWS), 0) + 64 * j == slot)
        store_slabs(dst, j, matmul(chosen, rows_ref[...]).astype(BF), mix)
        return carry

    lax.fori_loop(0, 8, step, 0)


def unpack(src, dst, unmix):
    def step(j, carry):
        dst[pl.ds(pl.multiple_of(64 * j, 64), 64), :] = load_slabs(src, j, unmix)
        return carry

    lax.fori_loop(0, 8, step, 0)


def attend_pair(queries, keys, values, bias):
    lane = iota((1, PAIR), 1)
    widened = jnp.concatenate([values, jnp.ones_like(values)], axis=1)
    outs = []
    for half in range(2):
        scores = matmul_nt(queries * ones_where((lane >= 64) == (half == 1)), keys)
        if bias is not None:
            scores = scores + bias
        powers = jnp.exp(scores - jnp.max(scores, axis=-1, keepdims=True)).astype(BF)
        both = matmul(powers, widened)
        outs.append(both[:, :PAIR] / both[:, PAIR:])
    return jnp.where(lane < 64, outs[0], outs[1]).astype(BF)


def kernel(
    grid_hbm, mesh_hbm, encode_block, decode_block, neighbour_block,
    encode_grid_gain, encode_mesh_gain, process_gain, decode_grid_gain, decode_mesh_gain,
    eq_hbm, ekv_hbm, eo_hbm, pqkv_hbm, po_hbm, dq_hbm, dkv_hbm, do_hbm,
    out_ref,
    grid, mesh, eq, ekv, eo, pqkv, po, dq, dkv, do,
    send1, recv1, send2, recv2, send3, recv3, lab2d, lab_send, lab_recv,
    rows_a, rows_b, query, mid, cand, wide_rows, keyval, bias_e, bias_d,
    load_sems, send_sems, recv_sems, halo_sems,
):
    z, x, y, c = coordinates()
    me = lax.axis_index("gx") * 32 + lax.axis_index("gy")
    barrier = pltpu.get_barrier_semaphore()

    def greet(k, carry):
        pl.semaphore_signal(barrier, inc=1, device_id=peer(k, 1), device_id_type=MESH)
        return carry

    loads = [
        pltpu.make_async_copy(src, dst, load_sems.at[i])
        for i, (src, dst) in enumerate(
            (
                (grid_hbm, grid), (dq_hbm, dq), (mesh_hbm, mesh), (eq_hbm, eq), (ekv_hbm, ekv),
                (eo_hbm, eo), (pqkv_hbm, pqkv), (po_hbm, po), (dkv_hbm, dkv), (do_hbm, do),
            )
        )
    ]
    loads[0].start()
    lax.fori_loop(1, DEVICES, greet, 0)
    for load in loads[1:]:
        load.start()

    mix = interleave()
    e_matches, e_rank, e_slot = slot_plan(encode_block[...])
    d_matches, d_rank, d_slot = slot_plan(decode_block[...])
    lab2d[...] = label_table(e_matches, e_rank, encode_block[...], 0) + label_table(
        d_matches, d_rank, decode_block[...], CAP
    )

    def spread(k, carry):
        lab_send[k] = lab2d[pl.ds(k, 1), :]
        return carry

    lax.fori_loop(0, DEVICES, spread, 0)
    loads[0].wait()
    norm_into(grid, 0, rows_a, 0, encode_grid_gain)
    pack(rows_a, e_slot, send1, mix)
    pl.semaphore_wait(barrier, DEVICES - 1)

    def remote(src, dst, which, k, sign):
        return pltpu.make_async_remote_copy(
            src_ref=src.at[k], dst_ref=dst.at[k], send_sem=send_sems.at[which],
            recv_sem=recv_sems.at[which], device_id=peer(k, sign), device_id_type=MESH,
        )

    def send_first(k, carry):
        remote(send1, recv1, 0, k, 1).start()
        remote(lab_send, lab_recv, 1, k, 1).start()
        return carry

    lax.fori_loop(1, DEVICES, send_first, 0)

    loads[1].wait()
    norm_into(grid, 0, rows_a, 0, decode_grid_gain)

    def store_query(at, out):
        rows_b[:, at] = (out * 0.125).astype(BF)

    project(rows_a, dq, D, 0, store_query)
    pack(rows_b, d_slot, send2, mix)

    def send_second(k, carry):
        remote(send2, recv2, 2, k, 1).start()
        return carry

    lax.fori_loop(1, DEVICES, send_second, 0)

    def all_slabs(ref):
        return ref.at[pl.ds(1, DEVICES - 1)]

    def wait_for(ref, sem):
        view = all_slabs(ref)
        pltpu.make_async_copy(view, view, sem).wait()

    loads[2].wait()
    norm_into(mesh, 0, rows_a, 0, encode_mesh_gain)
    loads[3].wait()

    def store_mesh_query(at, out):
        query[:, at] = (out * 0.125).astype(BF)

    project(rows_a, eq, D, 0, store_mesh_query)
    unmix = separate()
    recv1[0] = send1[0]
    recv2[0] = send2[0]
    lab_recv[0] = lab_send[0]
    loads[4].wait()
    wait_for(recv1, recv_sems.at[0])
    unpack(recv1, wide_rows, unmix)

    def store_keyval(at, out):
        keyval[:, at] = out.astype(BF)

    project(wide_rows, ekv, 2 * D, 0, store_keyval)

    wait_for(lab_recv, recv_sems.at[1])

    def gather_labels(k, carry):
        lab2d[pl.ds(k, 1), :] = lab_recv[k]
        return carry

    lax.fori_loop(0, DEVICES, gather_labels, 0)
    table = lab2d[...].astype(BF)
    spread_lanes = matmul(table, ones_where(iota((PAIR, SLOTS), 0) == (iota((PAIR, SLOTS), 1) & 3)))
    key_label = jnp.sum(
        jnp.where(iota((DEVICES, SLOTS), 0) == (iota((DEVICES, SLOTS), 1) >> 2), spread_lanes, 0.0),
        axis=0,
        keepdims=True,
    )
    spread_rows = matmul(ones_where((iota((SLOTS, DEVICES), 0) >> 2) == iota((SLOTS, DEVICES), 1)), table)
    query_label = jnp.sum(
        jnp.where(
            iota((SLOTS, PAIR), 1) == CAP + (iota((SLOTS, PAIR), 0) & 3), spread_rows, 0.0
        ),
        axis=1,
        keepdims=True,
    )
    block_row = iota((8, SLOTS), 0).astype(F32)
    bias_e[...] = jnp.where(key_label == block_row + 1.0, 0.0, MASKED)
    key_block = (iota((SLOTS, ROWS), 1) >> 7).astype(F32)
    bias_d[...] = jnp.where(query_label == key_block + 1.0, 0.0, MASKED)

    def encode_pair(p, carry):
        at = pl.ds(pl.multiple_of(p * PAIR, PAIR), PAIR)
        upper = pl.ds(pl.multiple_of(D + p * PAIR, PAIR), PAIR)
        for block in range(2):
            here = pl.ds(block * BLOCK, BLOCK)
            rows_a[here, at] = attend_pair(
                query[here, at], keyval[:, at], keyval[:, upper], bias_e[pl.ds(block, 1), :]
            )
        return carry

    lax.fori_loop(0, HEADS // 2, encode_pair, 0)

    loads[5].wait()

    def store_mid(at, out):
        mid[:, at] = (mesh[:, at].astype(F32) + out).astype(BF)

    project(rows_a, eo, D, 0, store_mid)
    norm_into(mid, 0, cand, ROWS, process_gain)

    def neighbour(step, sem, to):
        there = lax.rem(me + step + DEVICES, DEVICES)
        return pltpu.make_async_remote_copy(
            src_ref=cand.at[pl.ds(ROWS, ROWS)], dst_ref=cand.at[pl.ds(to, ROWS)],
            send_sem=halo_sems.at[sem], recv_sem=halo_sems.at[sem + 1],
            device_id=(there // 32, lax.rem(there, 32)), device_id_type=MESH,
        )

    to_right = neighbour(1, 0, 0)
    to_left = neighbour(-1, 2, 2 * ROWS)
    to_right.start()
    to_left.start()

    loads[6].wait()

    def store_process_query(at, out):
        query[:, at] = (out * 0.125).astype(BF)

    def store_own(at, out):
        keyval[pl.ds(0, ROWS), at] = out.astype(BF)

    def store_other(at, out):
        keyval[pl.ds(ROWS, ROWS), at] = out.astype(BF)

    own = cand.at[pl.ds(ROWS, ROWS)]
    project(own, pqkv, D, 0, store_process_query)
    project(own, pqkv, 2 * D, D, store_own)
    to_right.wait()
    to_left.wait()
    for block in range(2):
        position = neighbour_block[pl.ds(block, 1), :] - 2 * me + 2
        picked = None
        for candidate in (block, block + 1, block + 3, block + 4):
            weight = ones_where(position == candidate)
            weight = jnp.concatenate([weight] * (D // PAIR), axis=1)
            term = cand[pl.ds(candidate * BLOCK, BLOCK), :] * weight
            picked = term if picked is None else picked + term
        rows_b[pl.ds(block * BLOCK, BLOCK), :] = picked
    project(rows_b, pqkv, 2 * D, D, store_other)

    def process_pair(p, carry):
        at = pl.ds(pl.multiple_of(p * PAIR, PAIR), PAIR)
        upper = pl.ds(pl.multiple_of(D + p * PAIR, PAIR), PAIR)
        for block in range(2):
            here = pl.ds(block * BLOCK, BLOCK)
            there = pl.ds(ROWS + block * BLOCK, BLOCK)
            rows_a[here, at] = attend_pair(
                query[here, at],
                jnp.concatenate([keyval[here, at], keyval[there, at]], axis=0),
                jnp.concatenate([keyval[here, upper], keyval[there, upper]], axis=0),
                None,
            )
        return carry

    lax.fori_loop(0, HEADS // 2, process_pair, 0)
    loads[7].wait()

    def store_mesh_out(at, out):
        rows_b[:, at] = (mid[:, at].astype(F32) + out).astype(BF)

    project(rows_a, po, D, 0, store_mesh_out)
    norm_into(rows_b, 0, rows_a, 0, decode_mesh_gain)
    loads[8].wait()
    project(rows_a, dkv, 2 * D, 0, store_own)

    wait_for(recv2, recv_sems.at[2])
    unpack(recv2, wide_rows, unmix)

    for chunk in range(4):
        here = pl.ds(chunk * BLOCK, BLOCK)

        def decode_pair(p, carry):
            at = pl.ds(pl.multiple_of(p * PAIR, PAIR), PAIR)
            upper = pl.ds(pl.multiple_of(D + p * PAIR, PAIR), PAIR)
            mine = pl.ds(0, ROWS)
            rows_a[pl.ds(0, BLOCK), at] = attend_pair(
                wide_rows[here, at], keyval[mine, at], keyval[mine, upper], bias_d[here, :]
            )
            return carry

        lax.fori_loop(0, HEADS // 2, decode_pair, 0)
        for j in range(2):
            store_slabs(send3, 2 * chunk + j, rows_a[pl.ds(64 * j, 64), :], mix)

        def send_third(k, carry):
            remote(send3, recv3, 3, k, -1).start()
            return carry

        lax.fori_loop(max(1, 32 * chunk), 32 * chunk + 32, send_third, 0)
    recv3[0] = send3[0]
    wait_for(send1, send_sems.at[0])
    wait_for(lab_send, send_sems.at[1])
    wait_for(send2, send_sems.at[2])
    wait_for(recv3, recv_sems.at[3])
    unpack(recv3, wide_rows, unmix)
    slot_column = jnp.sum(
        jnp.where(iota((ROWS, ROWS), 0) == iota((ROWS, ROWS), 1), d_slot, 0).astype(F32),
        axis=1,
        keepdims=True,
    )
    choose = ones_where(iota((ROWS, SLOTS), 1).astype(F32) == slot_column)
    rows_b[...] = matmul(choose, wide_rows[...]).astype(BF)
    loads[9].wait()

    def store_out(at, out):
        out_ref[:, at] = out.astype(BF)

    project(rows_b, do, D, 0, store_out)
    wait_for(send3, send_sems.at[3])


def on_device(
    grid_state, mesh_state, encode_block, neighbour_block, decode_block,
    encode_grid_gain, encode_mesh_gain, process_gain, decode_grid_gain, decode_mesh_gain,
    encode_query, encode_keyval, encode_out, process_qkv, process_out,
    decode_query, decode_keyval, decode_out,
):
    hbm = pl.BlockSpec(memory_space=pl.ANY)
    vmem = pl.BlockSpec(memory_space=pltpu.VMEM)
    slabs = pltpu.VMEM((DEVICES, 16, 256), BF)
    rows = pltpu.VMEM((ROWS, D), BF)
    return pl.pallas_call(
        kernel,
        out_shape=jax.ShapeDtypeStruct((ROWS, D), BF),
        in_specs=[hbm, hbm, vmem, vmem, vmem] + [vmem] * 5 + [hbm] * 8,
        out_specs=vmem,
        scratch_shapes=[
            rows, rows,
            pltpu.VMEM((D, D), BF), pltpu.VMEM((D, 2 * D), BF), pltpu.VMEM((D, D), BF),
            pltpu.VMEM((D, 3 * D), BF), pltpu.VMEM((D, D), BF), pltpu.VMEM((D, D), BF),
            pltpu.VMEM((D, 2 * D), BF), pltpu.VMEM((D, D), BF),
            slabs, slabs, slabs, slabs, slabs, slabs,
            pltpu.VMEM((DEVICES, PAIR), F32),
            pltpu.VMEM((DEVICES, 1, PAIR), F32), pltpu.VMEM((DEVICES, 1, PAIR), F32),
            rows, rows, rows, rows,
            pltpu.VMEM((3 * ROWS, D), BF), pltpu.VMEM((SLOTS, D), BF),
            pltpu.VMEM((SLOTS, 2 * D), BF),
            pltpu.VMEM((8, SLOTS), F32), pltpu.VMEM((SLOTS, ROWS), F32),
            pltpu.SemaphoreType.DMA((10,)), pltpu.SemaphoreType.DMA((4,)),
            pltpu.SemaphoreType.DMA((4,)), pltpu.SemaphoreType.DMA((4,)),
        ],
        compiler_params=pltpu.CompilerParams(
            collective_id=0, has_side_effects=True, vmem_limit_bytes=60 * 1024 * 1024
        ),
    )(
        grid_state, mesh_state, encode_block.reshape(1, -1), decode_block.reshape(1, -1),
        jnp.broadcast_to(neighbour_block[:, None], (2, PAIR)),
        *(
            gain.reshape(1, -1)
            for gain in (
                encode_grid_gain, encode_mesh_gain, process_gain, decode_grid_gain, decode_mesh_gain,
            )
        ),
        encode_query, encode_keyval, encode_out, process_qkv, process_out,
        decode_query, decode_keyval, decode_out,
    )


def solution(mesh):
    rows, split = P(("gx", "gy"), None), P(("gx", "gy"))
    return jax.shard_map(
        on_device,
        mesh=mesh,
        in_specs=(rows, rows, split, split, split) + (P(),) * 13,
        out_specs=rows,
        check_vma=False,
    )
```

```python
import math

import jax
import jax.numpy as jnp
from jax import lax
from jax.experimental import pallas as pl
from jax.experimental.pallas import tpu as pltpu
from jax.sharding import PartitionSpec as P

HEADS = 16
BLOCK = 128
CAP = 4
DEVICES = 128
D = 1024
ROWS = 256
SLOTS = DEVICES * CAP
PAIR = 128
MASKED = -1e30
SCORE_SCALE = 0.125 * math.log2(math.e)
MESH = pl.DeviceIdType.MESH
BF = jnp.bfloat16
F32 = jnp.float32


def coordinates():
    gy = lax.axis_index("gy")
    return lax.axis_index("gx"), gy // 8, lax.rem(gy // 2, 4), lax.rem(gy, 2)


def device_at(z, x, y, c):
    return lax.rem(z + 4, 4), lax.rem(x + 4, 4) * 8 + lax.rem(y + 4, 4) * 2 + lax.rem(c + 2, 2)


def peer(k, sign):
    z, x, y, c = coordinates()
    return device_at(
        z + sign * lax.rem(k // 16, 4),
        x + sign * lax.rem(k, 4),
        y + sign * lax.rem(k // 4, 4),
        c + sign * (k // 64),
    )


def iota(shape, dim):
    return lax.broadcasted_iota(jnp.int32, shape, dim)


def ones_where(condition, dtype=BF):
    return jnp.where(condition, 1.0, 0.0).astype(dtype)


def matmul(a, b):
    return jnp.dot(a, b, preferred_element_type=F32)


def matmul_nt(a, b):
    return lax.dot_general(a, b, (((1,), (1,)), ((), ())), preferred_element_type=F32)


def norm_into(src, src_row, dst, dst_row, gain_ref, rows=ROWS):
    def step(i, carry):
        wide = src[pl.ds(pl.multiple_of(src_row + i * 32, 32), 32), :].astype(F32)
        scale = lax.rsqrt(jnp.mean(wide * wide, axis=-1, keepdims=True) + 1e-6)
        dst[pl.ds(pl.multiple_of(dst_row + i * 32, 32), 32), :] = (
            wide * scale * gain_ref[...]
        ).astype(BF)
        return carry

    lax.fori_loop(0, rows // 32, step, 0)


def project(a_ref, w_ref, columns, first_column, epilogue, tile=512):
    def step(n, carry):
        at = pl.multiple_of(n * tile, tile)
        out = matmul(a_ref[...], w_ref[:, pl.ds(pl.multiple_of(first_column + at, tile), tile)])
        epilogue(pl.ds(at, tile), out)
        return carry

    lax.fori_loop(0, columns // tile, step, 0)


def slot_plan(blocks):
    z, x, y, c = coordinates()
    owner = blocks >> 1
    k = (
        (((owner >> 3) & 3) - x & 3)
        + 4 * (((owner >> 1) & 3) - y & 3)
        + 16 * ((owner >> 5) - z & 3)
        + 64 * ((owner & 1) - c & 1)
    )
    matches = ones_where(iota((DEVICES, ROWS), 0) == k)
    earlier = ones_where(iota((ROWS, ROWS), 0) < iota((ROWS, ROWS), 1))
    counts = matmul(matches, earlier)
    rank = jnp.sum(matches.astype(F32) * counts, axis=0, keepdims=True).astype(jnp.int32)
    return matches, rank, k * CAP + rank


def label_table(matches, rank, blocks, base):
    coded = jnp.where(iota((PAIR, ROWS), 0) == rank + base, (blocks & 1) + 1, 0)
    return matmul_nt(matches, coded.astype(F32).astype(BF))


def interleave():
    m = iota((256, 256), 0)
    return ones_where(iota((256, 256), 1) == 64 * ((m >> 2) & 3) + 4 * (m >> 4) + (m & 3))


def separate():
    n = iota((256, 256), 0)
    return ones_where(iota((256, 256), 1) == 16 * ((n >> 2) & 15) + 4 * (n >> 6) + (n & 3))


def store_slabs(dst, j, rows, mix):
    tall = jnp.concatenate([rows[:, 256 * q : 256 * q + 256] for q in range(4)], axis=0)
    dst[pl.ds(16 * j, 16)] = matmul(mix, tall).astype(BF).reshape(16, 16, 256)


def load_slabs(src, j, unmix):
    tall = matmul(unmix, src[pl.ds(16 * j, 16)].reshape(256, 256)).astype(BF)
    return jnp.concatenate([tall[64 * q : 64 * q + 64] for q in range(4)], axis=1)


def pack(rows_ref, slot, dst, mix, first, last):
    def step(j, carry):
        chosen = ones_where(iota((64, ROWS), 0) + 64 * j == slot)
        store_slabs(dst, j, matmul(chosen, rows_ref[...]).astype(BF), mix)
        return carry

    lax.fori_loop(first, last, step, 0)


def unpack(src, dst, unmix, first, last):
    def step(j, carry):
        dst[pl.ds(pl.multiple_of(64 * j, 64), 64), :] = load_slabs(src, j, unmix)
        return carry

    lax.fori_loop(first, last, step, 0)


def attend_pairs(pairs):
    lane = iota((1, PAIR), 1)
    scores, outs = [], []
    for queries, query_tag, keys, key_tag, values in pairs:
        if key_tag is not None:
            keys = jnp.concatenate([keys, key_tag], axis=1)
        for half in range(2):
            part = queries * ones_where((lane >= 64) == (half == 1))
            if query_tag is not None:
                part = jnp.concatenate([part, query_tag], axis=1)
            scores.append(matmul_nt(part, keys))
    powers = [jnp.exp2(x - jnp.max(x, axis=-1, keepdims=True)).astype(BF) for x in scores]
    for i, (_, _, _, _, values) in enumerate(pairs):
        widened = jnp.concatenate([values, jnp.ones_like(values)], axis=1)
        halves = [matmul(powers[2 * i + half], widened) for half in range(2)]
        halves = [both[:, :PAIR] / both[:, PAIR:] for both in halves]
        outs.append(jnp.where(lane < 64, halves[0], halves[1]).astype(BF))
    return outs


def kernel(
    grid_hbm, mesh_hbm, encode_block, decode_block, neighbour_block,
    encode_grid_gain, encode_mesh_gain, process_gain, decode_grid_gain, decode_mesh_gain,
    eq_hbm, ekv_hbm, eo_hbm, pqkv_hbm, po_hbm, dq_hbm, dkv_hbm, do_hbm,
    out_ref,
    grid, mesh, eq, ekv, eo, pqkv, po, dq, dkv, do,
    send1, recv1, send2, recv2, send3, recv3, lab2d, lab_send, lab_recv,
    rows_a, rows_b, query, mid, cand, wide_rows, keyval, key_tags, query_tags,
    load_sems, send_sems, recv_sems, halo_sems,
):
    z, x, y, c = coordinates()
    me = lax.axis_index("gx") * 32 + lax.axis_index("gy")
    barrier = pltpu.get_barrier_semaphore()

    def greet(k, carry):
        pl.semaphore_signal(barrier, inc=1, device_id=peer(k, 1), device_id_type=MESH)
        return carry

    loads = [
        pltpu.make_async_copy(src, dst, load_sems.at[i])
        for i, (src, dst) in enumerate(
            (
                (grid_hbm, grid), (dq_hbm, dq), (mesh_hbm, mesh), (eq_hbm, eq), (ekv_hbm, ekv),
                (eo_hbm, eo), (pqkv_hbm, pqkv), (po_hbm, po), (dkv_hbm, dkv), (do_hbm, do),
            )
        )
    ]
    loads[0].start()
    lax.fori_loop(1, DEVICES, greet, 0)
    for load in loads[1:]:
        load.start()

    def remote(src, dst, sent, received, k, sign):
        return pltpu.make_async_remote_copy(
            src_ref=src.at[k], dst_ref=dst.at[k], send_sem=send_sems.at[sent],
            recv_sem=recv_sems.at[received], device_id=peer(k, sign), device_id_type=MESH,
        )

    def send_range(src, dst, sent, received, first, last, sign):
        def send(k, carry):
            remote(src, dst, sent, received, k, sign).start()
            return carry

        lax.fori_loop(max(1, first), last, send, 0)

    def wait_for(ref, first, last, sem):
        view = ref.at[pl.ds(max(1, first), last - max(1, first))]
        pltpu.make_async_copy(view, view, sem).wait()

    mix, unmix = interleave(), separate()
    e_matches, e_rank, e_slot = slot_plan(encode_block[...])
    loads[0].wait()
    norm_into(grid, 0, rows_a, 0, encode_grid_gain)
    pack(rows_a, e_slot, send1, mix, 0, 4)
    pl.semaphore_wait(barrier, DEVICES - 1)
    send_range(send1, recv1, 0, 0, 0, 64, 1)
    pack(rows_a, e_slot, send1, mix, 4, 8)
    send_range(send1, recv1, 0, 1, 64, 128, 1)

    d_matches, d_rank, d_slot = slot_plan(decode_block[...])
    lab2d[...] = label_table(e_matches, e_rank, encode_block[...], 0) + label_table(
        d_matches, d_rank, decode_block[...], CAP
    )

    def spread(k, carry):
        lab_send[k] = lab2d[pl.ds(k, 1), :]
        return carry

    lax.fori_loop(0, DEVICES, spread, 0)
    norm_into(grid, 0, rows_a, 0, decode_grid_gain)
    send_range(lab_send, lab_recv, 1, 2, 0, 128, 1)

    loads[1].wait()

    def store_query(at, out):
        rows_b[:, at] = (out * SCORE_SCALE).astype(BF)

    project(rows_a, dq, D, 0, store_query)
    pack(rows_b, d_slot, send2, mix, 0, 8)
    for group in range(2):
        send_range(send2, recv2, 2, 3 + group, 32 * group, 32 * group + 32, 1)

    loads[2].wait()
    norm_into(mesh, 0, rows_a, 0, encode_mesh_gain)
    loads[3].wait()

    def store_mesh_query(at, out):
        query[:, at] = (out * SCORE_SCALE).astype(BF)

    project(rows_a, eq, D, 0, store_mesh_query)
    recv1[0] = send1[0]
    recv2[0] = send2[0]
    lab_recv[0] = lab_send[0]
    loads[4].wait()
    for group in range(2):
        wait_for(recv1, 64 * group, 64 * group + 64, recv_sems.at[group])
        unpack(recv1, wide_rows, unmix, 4 * group, 4 * group + 4)
        part = pl.ds(group * ROWS, ROWS)

        def store_keyval(at, out):
            keyval[part, at] = out.astype(BF)

        project(wide_rows.at[part], ekv, 2 * D, 0, store_keyval)

    wait_for(lab_recv, 0, DEVICES, recv_sems.at[2])

    def gather_labels(k, carry):
        lab2d[pl.ds(k, 1), :] = lab_recv[k]
        return carry

    lax.fori_loop(0, DEVICES, gather_labels, 0)
    spread_rows = matmul(
        ones_where((iota((SLOTS, DEVICES), 0) >> 2) == iota((SLOTS, DEVICES), 1)),
        lab2d[...].astype(BF),
    )
    slot_lane = iota((SLOTS, PAIR), 1)
    slot_rank = iota((SLOTS, PAIR), 0) & 3

    def slot_tags(base):
        label = jnp.sum(
            jnp.where(slot_lane == base + slot_rank, spread_rows, 0.0), axis=1, keepdims=True
        )
        other = label != (slot_lane + 1).astype(F32)
        return jnp.where(other & (slot_lane < 2), MASKED, 0.0).astype(BF)

    key_tags[...] = slot_tags(0)
    query_tags[...] = slot_tags(CAP)

    def pair_at(p):
        return (
            pl.ds(pl.multiple_of(p * PAIR, PAIR), PAIR),
            pl.ds(pl.multiple_of(D + p * PAIR, PAIR), PAIR),
        )

    def halo(block, step, sem, to):
        there = lax.rem(me + step + DEVICES, DEVICES)
        return pltpu.make_async_remote_copy(
            src_ref=cand.at[pl.ds(ROWS + block * BLOCK, BLOCK)],
            dst_ref=cand.at[pl.ds(to + block * BLOCK, BLOCK)],
            send_sem=halo_sems.at[sem], recv_sem=halo_sems.at[sem + 1],
            device_id=(there // 32, lax.rem(there, 32)), device_id_type=MESH,
        )

    halos = []
    loads[5].wait()
    for block in range(2):
        here = pl.ds(block * BLOCK, BLOCK)
        block_tag = ones_where(iota((BLOCK, PAIR), 1) == block)

        def encode_pairs(g, carry):
            spots = [pair_at(4 * g + i) for i in range(4)]
            outs = attend_pairs(
                [
                    (query[here, at], block_tag, keyval[:, at], key_tags[...], keyval[:, upper])
                    for at, upper in spots
                ]
            )
            for (at, _), out in zip(spots, outs):
                rows_a[here, at] = out
            return carry

        lax.fori_loop(0, 2, encode_pairs, 0)

        def store_mid(at, out):
            mid[here, at] = (mesh[here, at].astype(F32) + out).astype(BF)

        project(rows_a.at[here], eo, D, 0, store_mid)
        norm_into(mid, block * BLOCK, cand, ROWS + block * BLOCK, process_gain, BLOCK)
        for step, sem, to in ((1, 4 * block, 0), (-1, 4 * block + 2, 2 * ROWS)):
            halos.append(halo(block, step, sem, to))
            halos[-1].start()
    for group in range(2, 4):
        send_range(send2, recv2, 2, 3 + group, 32 * group, 32 * group + 32, 1)

    loads[6].wait()

    def store_process_query(at, out):
        query[:, at] = (out * SCORE_SCALE).astype(BF)

    def store_own(at, out):
        keyval[pl.ds(0, ROWS), at] = out.astype(BF)

    def store_other(at, out):
        keyval[pl.ds(ROWS, ROWS), at] = out.astype(BF)

    own = cand.at[pl.ds(ROWS, ROWS)]
    project(own, pqkv, D, 0, store_process_query)
    project(own, pqkv, 2 * D, D, store_own)
    for copy in halos:
        copy.wait()
    for block in range(2):
        target = jnp.sum(
            jnp.where(iota((1, 2), 1) == block, neighbour_block[...], 0).astype(F32),
            axis=1,
            keepdims=True,
        )
        position = target - (2 * me - 2).astype(F32) + jnp.zeros((1, PAIR), F32)
        picked = None
        for candidate in (block, block + 1, block + 3, block + 4):
            weight = jnp.concatenate([ones_where(position == candidate)] * (D // PAIR), axis=1)
            term = cand[pl.ds(candidate * BLOCK, BLOCK), :] * weight
            picked = term if picked is None else picked + term
        rows_b[pl.ds(block * BLOCK, BLOCK), :] = picked
    project(rows_b, pqkv, 2 * D, D, store_other)

    def process_pairs(g, carry):
        spots = [(block, *pair_at(2 * g + i)) for i in range(2) for block in range(2)]
        work = []
        for block, at, upper in spots:
            here = pl.ds(block * BLOCK, BLOCK)
            there = pl.ds(ROWS + block * BLOCK, BLOCK)
            work.append(
                (
                    query[here, at], None,
                    jnp.concatenate([keyval[here, at], keyval[there, at]], axis=0), None,
                    jnp.concatenate([keyval[here, upper], keyval[there, upper]], axis=0),
                )
            )
        for (block, at, _), out in zip(spots, attend_pairs(work)):
            rows_a[pl.ds(block * BLOCK, BLOCK), at] = out
        return carry

    lax.fori_loop(0, HEADS // 4, process_pairs, 0)
    loads[7].wait()

    def store_mesh_out(at, out):
        rows_b[:, at] = (mid[:, at].astype(F32) + out).astype(BF)

    project(rows_a, po, D, 0, store_mesh_out)
    norm_into(rows_b, 0, rows_a, 0, decode_mesh_gain)
    loads[8].wait()
    project(rows_a, dkv, 2 * D, 0, store_own)

    node_tag = ones_where(iota((ROWS, PAIR), 1) == (iota((ROWS, PAIR), 0) >> 7))
    mine = pl.ds(0, ROWS)
    for chunk in range(4):
        here = pl.ds(chunk * BLOCK, BLOCK)
        wait_for(recv2, 32 * chunk, 32 * chunk + 32, recv_sems.at[3 + chunk])
        unpack(recv2, wide_rows, unmix, 2 * chunk, 2 * chunk + 2)

        def decode_pairs(g, carry):
            spots = [pair_at(4 * g + i) for i in range(4)]
            outs = attend_pairs(
                [
                    (
                        wide_rows[here, at], query_tags[here, :],
                        keyval[mine, at], node_tag, keyval[mine, upper],
                    )
                    for at, upper in spots
                ]
            )
            for (at, _), out in zip(spots, outs):
                rows_a[pl.ds(0, BLOCK), at] = out
            return carry

        lax.fori_loop(0, 2, decode_pairs, 0)
        for j in range(2):
            store_slabs(send3, 2 * chunk + j, rows_a[pl.ds(64 * j, 64), :], mix)
        send_range(send3, recv3, 3, 7 + chunk, 32 * chunk, 32 * chunk + 32, -1)
    recv3[0] = send3[0]
    slot_column = jnp.sum(
        jnp.where(iota((ROWS, ROWS), 0) == iota((ROWS, ROWS), 1), d_slot, 0).astype(F32),
        axis=1,
        keepdims=True,
    )
    wait_for(send1, 0, DEVICES, send_sems.at[0])
    wait_for(lab_send, 0, DEVICES, send_sems.at[1])
    wait_for(send2, 0, DEVICES, send_sems.at[2])
    decoded = None
    for chunk in range(4):
        choose = ones_where(
            (iota((ROWS, BLOCK), 1) + chunk * BLOCK).astype(F32) == slot_column
        )
        wait_for(recv3, 32 * chunk, 32 * chunk + 32, recv_sems.at[7 + chunk])
        unpack(recv3, wide_rows, unmix, 2 * chunk, 2 * chunk + 2)
        found = matmul(choose, wide_rows[pl.ds(chunk * BLOCK, BLOCK), :])
        decoded = found if decoded is None else decoded + found
    rows_b[...] = decoded.astype(BF)
    loads[9].wait()

    def store_out(at, out):
        out_ref[:, at] = out.astype(BF)

    project(rows_b, do, D, 0, store_out)
    wait_for(send3, 0, DEVICES, send_sems.at[3])


def on_device(
    grid_state, mesh_state, encode_block, neighbour_block, decode_block,
    encode_grid_gain, encode_mesh_gain, process_gain, decode_grid_gain, decode_mesh_gain,
    encode_query, encode_keyval, encode_out, process_qkv, process_out,
    decode_query, decode_keyval, decode_out,
):
    hbm = pl.BlockSpec(memory_space=pl.ANY)
    vmem = pl.BlockSpec(memory_space=pltpu.VMEM)
    slabs = pltpu.VMEM((DEVICES, 16, 256), BF)
    rows = pltpu.VMEM((ROWS, D), BF)
    return pl.pallas_call(
        kernel,
        out_shape=jax.ShapeDtypeStruct((ROWS, D), BF),
        in_specs=[hbm, hbm, vmem, vmem, vmem] + [vmem] * 5 + [hbm] * 8,
        out_specs=vmem,
        scratch_shapes=[
            rows, rows,
            pltpu.VMEM((D, D), BF), pltpu.VMEM((D, 2 * D), BF), pltpu.VMEM((D, D), BF),
            pltpu.VMEM((D, 3 * D), BF), pltpu.VMEM((D, D), BF), pltpu.VMEM((D, D), BF),
            pltpu.VMEM((D, 2 * D), BF), pltpu.VMEM((D, D), BF),
            slabs, slabs, slabs, slabs, slabs, slabs,
            pltpu.VMEM((DEVICES, PAIR), F32),
            pltpu.VMEM((DEVICES, 1, PAIR), F32), pltpu.VMEM((DEVICES, 1, PAIR), F32),
            rows, rows, rows, rows,
            pltpu.VMEM((3 * ROWS, D), BF), pltpu.VMEM((SLOTS, D), BF),
            pltpu.VMEM((SLOTS, 2 * D), BF),
            pltpu.VMEM((SLOTS, PAIR), BF), pltpu.VMEM((SLOTS, PAIR), BF),
            pltpu.SemaphoreType.DMA((10,)), pltpu.SemaphoreType.DMA((4,)),
            pltpu.SemaphoreType.DMA((11,)), pltpu.SemaphoreType.DMA((8,)),
        ],
        compiler_params=pltpu.CompilerParams(
            collective_id=0, has_side_effects=True, vmem_limit_bytes=60 * 1024 * 1024
        ),
    )(
        grid_state, mesh_state, encode_block.reshape(1, -1), decode_block.reshape(1, -1),
        neighbour_block.reshape(1, -1),
        *(
            gain.reshape(1, -1)
            for gain in (
                encode_grid_gain, encode_mesh_gain, process_gain, decode_grid_gain, decode_mesh_gain,
            )
        ),
        encode_query, encode_keyval, encode_out, process_qkv, process_out,
        decode_query, decode_keyval, decode_out,
    )


def solution(mesh):
    rows, split = P(("gx", "gy"), None), P(("gx", "gy"))
    return jax.shard_map(
        on_device,
        mesh=mesh,
        in_specs=(rows, rows, split, split, split) + (P(),) * 13,
        out_specs=rows,
        check_vma=False,
    )
```

```python
import math

import jax
import jax.numpy as jnp
from jax import lax
from jax.experimental import pallas as pl
from jax.experimental.pallas import tpu as pltpu
from jax.sharding import PartitionSpec as P

HEADS = 16
BLOCK = 128
CAP = 4
DEVICES = 128
D = 1024
ROWS = 256
SLOTS = DEVICES * CAP
PAIR = 128
MASKED = -1e30
SCORE_SCALE = 0.125 * math.log2(math.e)
MESH = pl.DeviceIdType.MESH
BF = jnp.bfloat16
F32 = jnp.float32


def coordinates():
    gy = lax.axis_index("gy")
    return lax.axis_index("gx"), gy // 8, lax.rem(gy // 2, 4), lax.rem(gy, 2)


def each_peer(visit, core, first, last, sign):
    z, x, y, c = coordinates()
    columns = [lax.rem(x + i, 4) * 8 for i in range(4)]
    lines = [lax.rem(y + i, 4) * 2 for i in range(4)]
    side = c if core == 0 else 1 - c

    def plane(kz, start):
        gx = lax.rem(z + sign * kz + 4, 4)
        for ky in range(4):
            line = lines[sign * ky % 4] + side
            for kx in range(4):
                if kx + 4 * ky >= start:
                    visit(64 * core + 16 * kz + 4 * ky + kx, (gx, columns[sign * kx % 4] + line))

    if core == 0 and first == 0:
        plane(0, 1)
        first = 1

    def step(kz, carry):
        plane(kz, 0)
        return carry

    lax.fori_loop(first, last, step, 0)


def iota(shape, dim):
    return lax.broadcasted_iota(jnp.int32, shape, dim)


def ones_where(condition, dtype=BF):
    return jnp.where(condition, 1.0, 0.0).astype(dtype)


def matmul(a, b):
    return jnp.dot(a, b, preferred_element_type=F32)


def matmul_nt(a, b):
    return lax.dot_general(a, b, (((1,), (1,)), ((), ())), preferred_element_type=F32)


def norm_into(src, src_row, dst, dst_row, gain_ref, rows=ROWS):
    def step(i, carry):
        wide = src[pl.ds(pl.multiple_of(src_row + i * 32, 32), 32), :].astype(F32)
        scale = lax.rsqrt(jnp.mean(wide * wide, axis=-1, keepdims=True) + 1e-6)
        dst[pl.ds(pl.multiple_of(dst_row + i * 32, 32), 32), :] = (
            wide * scale * gain_ref[...]
        ).astype(BF)
        return carry

    lax.fori_loop(0, rows // 32, step, 0)


def project(a_ref, w_ref, columns, first_column, epilogue, tile=512):
    def step(n, carry):
        at = pl.multiple_of(n * tile, tile)
        out = matmul(a_ref[...], w_ref[:, pl.ds(pl.multiple_of(first_column + at, tile), tile)])
        epilogue(pl.ds(at, tile), out)
        return carry

    lax.fori_loop(0, columns // tile, step, 0)


def slot_plan(blocks):
    z, x, y, c = coordinates()
    owner = blocks >> 1
    k = (
        (((owner >> 3) & 3) - x & 3)
        + 4 * (((owner >> 1) & 3) - y & 3)
        + 16 * ((owner >> 5) - z & 3)
        + 64 * ((owner & 1) - c & 1)
    )
    matches = ones_where(iota((DEVICES, ROWS), 0) == k)
    earlier = ones_where(iota((ROWS, ROWS), 0) < iota((ROWS, ROWS), 1))
    counts = matmul(matches, earlier)
    rank = jnp.sum(matches.astype(F32) * counts, axis=0, keepdims=True).astype(jnp.int32)
    return matches, rank, k * CAP + rank


def label_table(matches, rank, blocks, base):
    coded = jnp.where(iota((PAIR, ROWS), 0) == rank + base, (blocks & 1) + 1, 0)
    return matmul_nt(matches, coded.astype(F32).astype(BF))


def interleave():
    m = iota((256, 256), 0)
    return ones_where(iota((256, 256), 1) == 64 * ((m >> 2) & 3) + 4 * (m >> 4) + (m & 3))


def separate():
    n = iota((256, 256), 0)
    return ones_where(iota((256, 256), 1) == 16 * ((n >> 2) & 15) + 4 * (n >> 6) + (n & 3))


def store_slabs(dst, j, rows, mix):
    tall = jnp.concatenate([rows[:, 256 * q : 256 * q + 256] for q in range(4)], axis=0)
    dst[pl.ds(16 * j, 16)] = matmul(mix, tall).astype(BF).reshape(16, 16, 256)


def load_slabs(src, j, unmix):
    tall = matmul(unmix, src[pl.ds(16 * j, 16)].reshape(256, 256)).astype(BF)
    return jnp.concatenate([tall[64 * q : 64 * q + 64] for q in range(4)], axis=1)


def pack(rows_ref, slot, dst, mix, half):
    chosen = ones_where(iota((ROWS, ROWS), 0) + ROWS * half == slot)
    rows = matmul(chosen, rows_ref[...]).astype(BF)
    for j in range(4):
        store_slabs(dst, 4 * half + j, rows[64 * j : 64 * j + 64], mix)


def unpack(src, dst, unmix, first, last):
    def step(j, carry):
        dst[pl.ds(pl.multiple_of(64 * j, 64), 64), :] = load_slabs(src, j, unmix)
        return carry

    lax.fori_loop(first, last, step, 0, unroll=True)


def attend_pairs(pairs):
    lane = iota((1, PAIR), 1)
    scores, outs = [], []
    for queries, query_tag, keys, key_tag, values in pairs:
        if key_tag is not None:
            keys = jnp.concatenate([keys, key_tag], axis=1)
        for half in range(2):
            part = queries * ones_where((lane >= 64) == (half == 1))
            if query_tag is not None:
                part = jnp.concatenate([part, query_tag], axis=1)
            scores.append(matmul_nt(part, keys))
    powers = [jnp.exp2(x - jnp.max(x, axis=-1, keepdims=True)).astype(BF) for x in scores]
    for i, (_, _, _, _, values) in enumerate(pairs):
        widened = jnp.concatenate([values, jnp.ones_like(values)], axis=1)
        halves = [matmul(powers[2 * i + half], widened) for half in range(2)]
        halves = [both[:, :PAIR] / both[:, PAIR:] for both in halves]
        outs.append(jnp.where(lane < 64, halves[0], halves[1]).astype(BF))
    return outs


def kernel(
    grid_hbm, mesh_hbm, encode_block, decode_block, neighbour_block,
    encode_grid_gain, encode_mesh_gain, process_gain, decode_grid_gain, decode_mesh_gain,
    eq_hbm, ekv_hbm, eo_hbm, pqkv_hbm, po_hbm, dq_hbm, dkv_hbm, do_hbm,
    out_ref,
    grid, mesh, eq, ekv, eo, pqkv, po, dq, dkv, do,
    send1, recv1, send2, recv2, send3, recv3, lab2d, lab_send, lab_recv,
    rows_a, rows_b, query, mid, cand, wide_rows, keyval, key_tags, query_tags,
    load_sems, send_sems, recv_sems, halo_sems,
):
    z, x, y, c = coordinates()
    me = lax.axis_index("gx") * 32 + lax.axis_index("gy")
    barrier = pltpu.get_barrier_semaphore()

    def greet(k, device):
        pl.semaphore_signal(barrier, inc=1, device_id=device, device_id_type=MESH)

    loads = [
        pltpu.make_async_copy(src, dst, load_sems.at[i])
        for i, (src, dst) in enumerate(
            (
                (grid_hbm, grid), (dq_hbm, dq), (mesh_hbm, mesh), (eq_hbm, eq), (ekv_hbm, ekv),
                (eo_hbm, eo), (pqkv_hbm, pqkv), (po_hbm, po), (dkv_hbm, dkv), (do_hbm, do),
            )
        )
    ]
    loads[0].start()
    each_peer(greet, 0, 0, 4, 1)
    each_peer(greet, 1, 0, 4, 1)
    for load in loads[1:]:
        load.start()

    def send_planes(src, dst, sent, received, core, first, last, sign):
        def send(k, device):
            pltpu.make_async_remote_copy(
                src_ref=src.at[k], dst_ref=dst.at[k], send_sem=send_sems.at[sent],
                recv_sem=recv_sems.at[received], device_id=device, device_id_type=MESH,
            ).start()

        each_peer(send, core, first, last, sign)

    def wait_for(ref, first, last, sem):
        view = ref.at[pl.ds(max(1, first), last - max(1, first))]
        pltpu.make_async_copy(view, view, sem).wait()

    mix, unmix = interleave(), separate()
    e_matches, e_rank, e_slot = slot_plan(encode_block[...])
    loads[0].wait()
    norm_into(grid, 0, rows_a, 0, encode_grid_gain)
    pack(rows_a, e_slot, send1, mix, 0)
    pl.semaphore_wait(barrier, DEVICES - 1)
    send_planes(send1, recv1, 0, 0, 0, 0, 4, 1)
    pack(rows_a, e_slot, send1, mix, 1)
    send_planes(send1, recv1, 0, 1, 1, 0, 4, 1)

    d_matches, d_rank, d_slot = slot_plan(decode_block[...])
    lab2d[...] = label_table(e_matches, e_rank, encode_block[...], 0) + label_table(
        d_matches, d_rank, decode_block[...], CAP
    )

    def spread(k, carry):
        lab_send[k] = lab2d[pl.ds(k, 1), :]
        return carry

    lax.fori_loop(0, DEVICES, spread, 0, unroll=8)
    norm_into(grid, 0, rows_a, 0, decode_grid_gain)
    for core in range(2):
        send_planes(lab_send, lab_recv, 1, 2, core, 0, 4, 1)

    loads[1].wait()

    def store_query(at, out):
        rows_b[:, at] = (out * SCORE_SCALE).astype(BF)

    project(rows_a, dq, D, 0, store_query)
    pack(rows_b, d_slot, send2, mix, 0)
    for group in range(2):
        send_planes(send2, recv2, 2, 3 + group, 0, 2 * group, 2 * group + 2, 1)
    pack(rows_b, d_slot, send2, mix, 1)

    loads[2].wait()
    norm_into(mesh, 0, rows_a, 0, encode_mesh_gain)
    loads[3].wait()

    def store_mesh_query(at, out):
        query[:, at] = (out * SCORE_SCALE).astype(BF)

    project(rows_a, eq, D, 0, store_mesh_query)
    recv1[0] = send1[0]
    recv2[0] = send2[0]
    lab_recv[0] = lab_send[0]
    loads[4].wait()
    for group in range(2):
        wait_for(recv1, 64 * group, 64 * group + 64, recv_sems.at[group])
        unpack(recv1, wide_rows, unmix, 4 * group, 4 * group + 4)
        part = pl.ds(group * ROWS, ROWS)

        def store_keyval(at, out):
            keyval[part, at] = out.astype(BF)

        project(wide_rows.at[part], ekv, 2 * D, 0, store_keyval)

    wait_for(lab_recv, 0, DEVICES, recv_sems.at[2])

    def gather_labels(k, carry):
        lab2d[pl.ds(k, 1), :] = lab_recv[k]
        return carry

    lax.fori_loop(0, DEVICES, gather_labels, 0, unroll=8)
    spread_rows = matmul(
        ones_where((iota((SLOTS, DEVICES), 0) >> 2) == iota((SLOTS, DEVICES), 1)),
        lab2d[...].astype(BF),
    )
    slot_lane = iota((SLOTS, PAIR), 1)
    slot_rank = iota((SLOTS, PAIR), 0) & 3

    def slot_tags(base):
        label = jnp.sum(
            jnp.where(slot_lane == base + slot_rank, spread_rows, 0.0), axis=1, keepdims=True
        )
        other = label != (slot_lane + 1).astype(F32)
        return jnp.where(other & (slot_lane < 2), MASKED, 0.0).astype(BF)

    key_tags[...] = slot_tags(0)
    query_tags[...] = slot_tags(CAP)

    def pair_at(p):
        return (
            pl.ds(pl.multiple_of(p * PAIR, PAIR), PAIR),
            pl.ds(pl.multiple_of(D + p * PAIR, PAIR), PAIR),
        )

    def halo(block, step, sem, to):
        there = lax.rem(me + step + DEVICES, DEVICES)
        return pltpu.make_async_remote_copy(
            src_ref=cand.at[pl.ds(ROWS + block * BLOCK, BLOCK)],
            dst_ref=cand.at[pl.ds(to + block * BLOCK, BLOCK)],
            send_sem=halo_sems.at[sem], recv_sem=halo_sems.at[sem + 1],
            device_id=(there // 32, lax.rem(there, 32)), device_id_type=MESH,
        )

    halos = []
    loads[5].wait()
    for block in range(2):
        here = pl.ds(block * BLOCK, BLOCK)
        block_tag = ones_where(iota((BLOCK, PAIR), 1) == block)

        def encode_pairs(g, carry):
            spots = [pair_at(4 * g + i) for i in range(4)]
            outs = attend_pairs(
                [
                    (query[here, at], block_tag, keyval[:, at], key_tags[...], keyval[:, upper])
                    for at, upper in spots
                ]
            )
            for (at, _), out in zip(spots, outs):
                rows_a[here, at] = out
            return carry

        lax.fori_loop(0, 2, encode_pairs, 0)

        def store_mid(at, out):
            mid[here, at] = (mesh[here, at].astype(F32) + out).astype(BF)

        project(rows_a.at[here], eo, D, 0, store_mid)
        norm_into(mid, block * BLOCK, cand, ROWS + block * BLOCK, process_gain, BLOCK)
        for step, sem, to in ((1, 4 * block, 0), (-1, 4 * block + 2, 2 * ROWS)):
            halos.append(halo(block, step, sem, to))
            halos[-1].start()
    for group in range(2):
        send_planes(send2, recv2, 2, 5 + group, 1, 2 * group, 2 * group + 2, 1)

    loads[6].wait()

    def store_process_query(at, out):
        query[:, at] = (out * SCORE_SCALE).astype(BF)

    def store_own(at, out):
        keyval[pl.ds(0, ROWS), at] = out.astype(BF)

    def store_other(at, out):
        keyval[pl.ds(ROWS, ROWS), at] = out.astype(BF)

    own = cand.at[pl.ds(ROWS, ROWS)]
    project(own, pqkv, D, 0, store_process_query)
    project(own, pqkv, 2 * D, D, store_own)
    for copy in halos:
        copy.wait()
    for block in range(2):
        target = jnp.sum(
            jnp.where(iota((1, 2), 1) == block, neighbour_block[...], 0).astype(F32),
            axis=1,
            keepdims=True,
        )
        position = target - (2 * me - 2).astype(F32) + jnp.zeros((1, PAIR), F32)
        picked = None
        for candidate in (block, block + 1, block + 3, block + 4):
            weight = jnp.concatenate([ones_where(position == candidate)] * (D // PAIR), axis=1)
            term = cand[pl.ds(candidate * BLOCK, BLOCK), :] * weight
            picked = term if picked is None else picked + term
        rows_b[pl.ds(block * BLOCK, BLOCK), :] = picked
    project(rows_b, pqkv, 2 * D, D, store_other)

    def process_pairs(g, carry):
        spots = [(block, *pair_at(2 * g + i)) for i in range(2) for block in range(2)]
        work = []
        for block, at, upper in spots:
            here = pl.ds(block * BLOCK, BLOCK)
            there = pl.ds(ROWS + block * BLOCK, BLOCK)
            work.append(
                (
                    query[here, at], None,
                    jnp.concatenate([keyval[here, at], keyval[there, at]], axis=0), None,
                    jnp.concatenate([keyval[here, upper], keyval[there, upper]], axis=0),
                )
            )
        for (block, at, _), out in zip(spots, attend_pairs(work)):
            rows_a[pl.ds(block * BLOCK, BLOCK), at] = out
        return carry

    lax.fori_loop(0, HEADS // 4, process_pairs, 0)
    loads[7].wait()

    def store_mesh_out(at, out):
        rows_b[:, at] = (mid[:, at].astype(F32) + out).astype(BF)

    project(rows_a, po, D, 0, store_mesh_out)
    norm_into(rows_b, 0, rows_a, 0, decode_mesh_gain)
    loads[8].wait()
    project(rows_a, dkv, 2 * D, 0, store_own)

    node_tag = ones_where(iota((ROWS, PAIR), 1) == (iota((ROWS, PAIR), 0) >> 7))
    mine = pl.ds(0, ROWS)
    for chunk in range(4):
        here = pl.ds(chunk * BLOCK, BLOCK)
        wait_for(recv2, 32 * chunk, 32 * chunk + 32, recv_sems.at[3 + chunk])
        unpack(recv2, wide_rows, unmix, 2 * chunk, 2 * chunk + 2)

        def decode_pairs(g, carry):
            spots = [pair_at(4 * g + i) for i in range(4)]
            outs = attend_pairs(
                [
                    (
                        wide_rows[here, at], query_tags[here, :],
                        keyval[mine, at], node_tag, keyval[mine, upper],
                    )
                    for at, upper in spots
                ]
            )
            for (at, _), out in zip(spots, outs):
                rows_a[pl.ds(0, BLOCK), at] = out
            return carry

        lax.fori_loop(0, 2, decode_pairs, 0)
        for j in range(2):
            store_slabs(send3, 2 * chunk + j, rows_a[pl.ds(64 * j, 64), :], mix)
        send_planes(send3, recv3, 3, 7 + chunk, chunk // 2, chunk % 2 * 2, chunk % 2 * 2 + 2, -1)
    recv3[0] = send3[0]
    slot_column = jnp.sum(
        jnp.where(iota((ROWS, ROWS), 0) == iota((ROWS, ROWS), 1), d_slot, 0).astype(F32),
        axis=1,
        keepdims=True,
    )
    wait_for(send1, 0, DEVICES, send_sems.at[0])
    wait_for(lab_send, 0, DEVICES, send_sems.at[1])
    wait_for(send2, 0, DEVICES, send_sems.at[2])
    decoded = None
    for chunk in range(4):
        choose = ones_where(
            (iota((ROWS, BLOCK), 1) + chunk * BLOCK).astype(F32) == slot_column
        )
        wait_for(recv3, 32 * chunk, 32 * chunk + 32, recv_sems.at[7 + chunk])
        unpack(recv3, wide_rows, unmix, 2 * chunk, 2 * chunk + 2)
        found = matmul(choose, wide_rows[pl.ds(chunk * BLOCK, BLOCK), :])
        decoded = found if decoded is None else decoded + found
    rows_b[...] = decoded.astype(BF)
    loads[9].wait()

    def store_out(at, out):
        out_ref[:, at] = out.astype(BF)

    project(rows_b, do, D, 0, store_out)
    wait_for(send3, 0, DEVICES, send_sems.at[3])


def on_device(
    grid_state, mesh_state, encode_block, neighbour_block, decode_block,
    encode_grid_gain, encode_mesh_gain, process_gain, decode_grid_gain, decode_mesh_gain,
    encode_query, encode_keyval, encode_out, process_qkv, process_out,
    decode_query, decode_keyval, decode_out,
):
    hbm = pl.BlockSpec(memory_space=pl.ANY)
    vmem = pl.BlockSpec(memory_space=pltpu.VMEM)
    slabs = pltpu.VMEM((DEVICES, 16, 256), BF)
    rows = pltpu.VMEM((ROWS, D), BF)
    return pl.pallas_call(
        kernel,
        out_shape=jax.ShapeDtypeStruct((ROWS, D), BF),
        in_specs=[hbm, hbm, vmem, vmem, vmem] + [vmem] * 5 + [hbm] * 8,
        out_specs=vmem,
        scratch_shapes=[
            rows, rows,
            pltpu.VMEM((D, D), BF), pltpu.VMEM((D, 2 * D), BF), pltpu.VMEM((D, D), BF),
            pltpu.VMEM((D, 3 * D), BF), pltpu.VMEM((D, D), BF), pltpu.VMEM((D, D), BF),
            pltpu.VMEM((D, 2 * D), BF), pltpu.VMEM((D, D), BF),
            slabs, slabs, slabs, slabs, slabs, slabs,
            pltpu.VMEM((DEVICES, PAIR), F32),
            pltpu.VMEM((DEVICES, 1, PAIR), F32), pltpu.VMEM((DEVICES, 1, PAIR), F32),
            rows, rows, rows, rows,
            pltpu.VMEM((3 * ROWS, D), BF), pltpu.VMEM((SLOTS, D), BF),
            pltpu.VMEM((SLOTS, 2 * D), BF),
            pltpu.VMEM((SLOTS, PAIR), BF), pltpu.VMEM((SLOTS, PAIR), BF),
            pltpu.SemaphoreType.DMA((10,)), pltpu.SemaphoreType.DMA((4,)),
            pltpu.SemaphoreType.DMA((11,)), pltpu.SemaphoreType.DMA((8,)),
        ],
        compiler_params=pltpu.CompilerParams(
            collective_id=0, has_side_effects=True, vmem_limit_bytes=60 * 1024 * 1024
        ),
    )(
        grid_state, mesh_state, encode_block.reshape(1, -1), decode_block.reshape(1, -1),
        neighbour_block.reshape(1, -1),
        *(
            gain.reshape(1, -1)
            for gain in (
                encode_grid_gain, encode_mesh_gain, process_gain, decode_grid_gain, decode_mesh_gain,
            )
        ),
        encode_query, encode_keyval, encode_out, process_qkv, process_out,
        decode_query, decode_keyval, decode_out,
    )


def solution(mesh):
    rows, split = P(("gx", "gy"), None), P(("gx", "gy"))
    return jax.shard_map(
        on_device,
        mesh=mesh,
        in_specs=(rows, rows, split, split, split) + (P(),) * 13,
        out_specs=rows,
        check_vma=False,
    )
```

```python
import math

import jax
import jax.numpy as jnp
from jax import lax
from jax.experimental import pallas as pl
from jax.experimental.pallas import tpu as pltpu
from jax.sharding import PartitionSpec as P

HEADS = 16
BLOCK = 128
CAP = 4
DEVICES = 128
D = 1024
ROWS = 256
SLOTS = DEVICES * CAP
PAIR = 128
MASKED = -1e30
SCORE_SCALE = 0.125 * math.log2(math.e)
MESH = pl.DeviceIdType.MESH
BF = jnp.bfloat16
F32 = jnp.float32


def coordinates():
    gy = lax.axis_index("gy")
    return lax.axis_index("gx"), gy // 8, lax.rem(gy // 2, 4), lax.rem(gy, 2)


def each_peer(visit, core, first, last, sign):
    z, x, y, c = coordinates()
    columns = [lax.rem(x + i, 4) * 8 for i in range(4)]
    lines = [lax.rem(y + i, 4) * 2 for i in range(4)]
    side = c if core == 0 else 1 - c

    def plane(kz, start):
        gx = lax.rem(z + sign * kz + 4, 4)
        for ky in range(4):
            line = lines[sign * ky % 4] + side
            for kx in range(4):
                if kx + 4 * ky >= start:
                    visit(64 * core + 16 * kz + 4 * ky + kx, (gx, columns[sign * kx % 4] + line))

    if core == 0 and first == 0:
        plane(0, 1)
        first = 1

    def step(kz, carry):
        plane(kz, 0)
        return carry

    lax.fori_loop(first, last, step, 0)


def iota(shape, dim):
    return lax.broadcasted_iota(jnp.int32, shape, dim)


def ones_where(condition, dtype=BF):
    return jnp.where(condition, 1.0, 0.0).astype(dtype)


def matmul(a, b):
    return jnp.dot(a, b, preferred_element_type=F32)


def matmul_nt(a, b):
    return lax.dot_general(a, b, (((1,), (1,)), ((), ())), preferred_element_type=F32)


def norm_into(src, src_row, dst, dst_row, gain_ref, rows=ROWS):
    def step(i, carry):
        wide = src[pl.ds(pl.multiple_of(src_row + i * 32, 32), 32), :].astype(F32)
        scale = lax.rsqrt(jnp.mean(wide * wide, axis=-1, keepdims=True) + 1e-6)
        dst[pl.ds(pl.multiple_of(dst_row + i * 32, 32), 32), :] = (
            wide * scale * gain_ref[...]
        ).astype(BF)
        return carry

    lax.fori_loop(0, rows // 32, step, 0)


def project(a_ref, w_ref, columns, first_column, epilogue, tile=512):
    def step(n, carry):
        at = pl.multiple_of(n * tile, tile)
        out = matmul(a_ref[...], w_ref[:, pl.ds(pl.multiple_of(first_column + at, tile), tile)])
        epilogue(pl.ds(at, tile), out)
        return carry

    lax.fori_loop(0, columns // tile, step, 0, unroll=True)


def slot_plan(blocks):
    z, x, y, c = coordinates()
    owner = blocks >> 1
    k = (
        (((owner >> 3) & 3) - x & 3)
        + 4 * (((owner >> 1) & 3) - y & 3)
        + 16 * ((owner >> 5) - z & 3)
        + 64 * ((owner & 1) - c & 1)
    )
    matches = ones_where(iota((DEVICES, ROWS), 0) == k)
    earlier = ones_where(iota((ROWS, ROWS), 0) < iota((ROWS, ROWS), 1))
    counts = matmul(matches, earlier)
    rank = jnp.sum(matches.astype(F32) * counts, axis=0, keepdims=True).astype(jnp.int32)
    return matches, rank, k * CAP + rank


def label_table(matches, rank, blocks, base):
    coded = jnp.where(iota((PAIR, ROWS), 0) == rank + base, (blocks & 1) + 1, 0)
    return matmul_nt(matches, coded.astype(F32).astype(BF))


def interleave():
    m = iota((256, 256), 0)
    return ones_where(iota((256, 256), 1) == 64 * ((m >> 2) & 3) + 4 * (m >> 4) + (m & 3))


def separate():
    n = iota((256, 256), 0)
    return ones_where(iota((256, 256), 1) == 16 * ((n >> 2) & 15) + 4 * (n >> 6) + (n & 3))


def store_slabs(dst, j, rows, mix):
    tall = jnp.concatenate([rows[:, 256 * q : 256 * q + 256] for q in range(4)], axis=0)
    dst[pl.ds(16 * j, 16)] = matmul(mix, tall).astype(BF).reshape(16, 16, 256)


def load_slabs(src, j, unmix):
    tall = matmul(unmix, src[pl.ds(16 * j, 16)].reshape(256, 256)).astype(BF)
    return jnp.concatenate([tall[64 * q : 64 * q + 64] for q in range(4)], axis=1)


def pack(rows_ref, slot, dst, mix, half):
    chosen = ones_where(iota((ROWS, ROWS), 0) + ROWS * half == slot)
    rows = matmul(chosen, rows_ref[...]).astype(BF)
    for j in range(4):
        store_slabs(dst, 4 * half + j, rows[64 * j : 64 * j + 64], mix)


def unpack(src, dst, unmix, first, last):
    def step(j, carry):
        dst[pl.ds(pl.multiple_of(64 * j, 64), 64), :] = load_slabs(src, j, unmix)
        return carry

    lax.fori_loop(first, last, step, 0, unroll=True)


def attend_pairs(pairs):
    lane = iota((1, PAIR), 1)
    scores, outs = [], []
    for queries, query_tag, keys, key_tag, values in pairs:
        if key_tag is not None:
            keys = jnp.concatenate([keys, key_tag], axis=1)
        for half in range(2):
            part = queries * ones_where((lane >= 64) == (half == 1))
            if query_tag is not None:
                part = jnp.concatenate([part, query_tag], axis=1)
            scores.append(matmul_nt(part, keys))
    powers = [jnp.exp2(x - jnp.max(x, axis=-1, keepdims=True)).astype(BF) for x in scores]
    for i, (_, _, _, _, values) in enumerate(pairs):
        widened = jnp.concatenate([values, jnp.ones_like(values)], axis=1)
        halves = [matmul(powers[2 * i + half], widened) for half in range(2)]
        halves = [both[:, :PAIR] / both[:, PAIR:] for both in halves]
        outs.append(jnp.where(lane < 64, halves[0], halves[1]).astype(BF))
    return outs


def kernel(
    grid_hbm, mesh_hbm, encode_block, decode_block, neighbour_block,
    encode_grid_gain, encode_mesh_gain, process_gain, decode_grid_gain, decode_mesh_gain,
    eq_hbm, ekv_hbm, eo_hbm, pqkv_hbm, po_hbm, dq_hbm, dkv_hbm, do_hbm,
    out_ref,
    grid, mesh, eq, ekv, eo, pqkv, po, dq, dkv, do,
    send1, recv1, send2, recv2, send3, recv3, lab2d, lab_send, lab_recv,
    rows_a, rows_b, query, mid, cand, wide_rows, keyval, key_tags, query_tags,
    load_sems, send_sems, recv_sems, halo_sems,
):
    z, x, y, c = coordinates()
    me = lax.axis_index("gx") * 32 + lax.axis_index("gy")
    barrier = pltpu.get_barrier_semaphore()

    def greet(k, device):
        pl.semaphore_signal(barrier, inc=1, device_id=device, device_id_type=MESH)

    loads = [
        pltpu.make_async_copy(src, dst, load_sems.at[i])
        for i, (src, dst) in enumerate(
            (
                (grid_hbm, grid), (dq_hbm, dq), (mesh_hbm, mesh), (eq_hbm, eq), (ekv_hbm, ekv),
                (eo_hbm, eo), (pqkv_hbm, pqkv), (po_hbm, po), (dkv_hbm, dkv), (do_hbm, do),
            )
        )
    ]
    loads[0].start()
    each_peer(greet, 0, 0, 4, 1)
    each_peer(greet, 1, 0, 4, 1)
    for load in loads[1:]:
        load.start()

    def send_planes(src, dst, sent, received, core, first, last, sign):
        def send(k, device):
            pltpu.make_async_remote_copy(
                src_ref=src.at[k], dst_ref=dst.at[k], send_sem=send_sems.at[sent],
                recv_sem=recv_sems.at[received], device_id=device, device_id_type=MESH,
            ).start()

        each_peer(send, core, first, last, sign)

    def wait_for(ref, first, last, sem):
        view = ref.at[pl.ds(max(1, first), last - max(1, first))]
        pltpu.make_async_copy(view, view, sem).wait()

    mix, unmix = interleave(), separate()
    e_matches, e_rank, e_slot = slot_plan(encode_block[...])
    loads[0].wait()
    norm_into(grid, 0, rows_a, 0, encode_grid_gain)
    pack(rows_a, e_slot, send1, mix, 0)
    pl.semaphore_wait(barrier, DEVICES - 1)
    send_planes(send1, recv1, 0, 0, 0, 0, 4, 1)
    pack(rows_a, e_slot, send1, mix, 1)
    send_planes(send1, recv1, 0, 1, 1, 0, 4, 1)

    d_matches, d_rank, d_slot = slot_plan(decode_block[...])
    lab2d[...] = label_table(e_matches, e_rank, encode_block[...], 0) + label_table(
        d_matches, d_rank, decode_block[...], CAP
    )

    def spread(k, carry):
        lab_send[k] = lab2d[pl.ds(k, 1), :]
        return carry

    lax.fori_loop(0, DEVICES, spread, 0, unroll=8)
    norm_into(grid, 0, rows_a, 0, decode_grid_gain)
    for core in range(2):
        send_planes(lab_send, lab_recv, 1, 2, core, 0, 4, 1)

    loads[1].wait()

    def store_query(at, out):
        rows_b[:, at] = (out * SCORE_SCALE).astype(BF)

    project(rows_a, dq, D, 0, store_query)
    pack(rows_b, d_slot, send2, mix, 0)
    pack(rows_b, d_slot, send2, mix, 1)

    loads[2].wait()
    norm_into(mesh, 0, rows_a, 0, encode_mesh_gain)
    loads[3].wait()

    def store_mesh_query(at, out):
        query[:, at] = (out * SCORE_SCALE).astype(BF)

    project(rows_a, eq, D, 0, store_mesh_query)
    recv1[0] = send1[0]
    recv2[0] = send2[0]
    lab_recv[0] = lab_send[0]
    loads[4].wait()
    for group in range(2):
        wait_for(recv1, 64 * group, 64 * group + 64, recv_sems.at[group])
        unpack(recv1, wide_rows, unmix, 4 * group, 4 * group + 4)
        part = pl.ds(group * ROWS, ROWS)

        def store_keyval(at, out):
            keyval[part, at] = out.astype(BF)

        project(wide_rows.at[part], ekv, 2 * D, 0, store_keyval)

    wait_for(lab_recv, 0, DEVICES, recv_sems.at[2])

    def gather_labels(k, carry):
        lab2d[pl.ds(k, 1), :] = lab_recv[k]
        return carry

    lax.fori_loop(0, DEVICES, gather_labels, 0, unroll=8)
    spread_rows = matmul(
        ones_where((iota((SLOTS, DEVICES), 0) >> 2) == iota((SLOTS, DEVICES), 1)),
        lab2d[...].astype(BF),
    )
    slot_lane = iota((SLOTS, PAIR), 1)
    slot_rank = iota((SLOTS, PAIR), 0) & 3

    def slot_tags(base):
        label = jnp.sum(
            jnp.where(slot_lane == base + slot_rank, spread_rows, 0.0), axis=1, keepdims=True
        )
        other = label != (slot_lane + 1).astype(F32)
        return jnp.where(other & (slot_lane < 2), MASKED, 0.0).astype(BF)

    key_tags[...] = slot_tags(0)
    query_tags[...] = slot_tags(CAP)

    def pair_at(p):
        if isinstance(p, int):
            return pl.ds(p * PAIR, PAIR), pl.ds(D + p * PAIR, PAIR)
        return (
            pl.ds(pl.multiple_of(p * PAIR, PAIR), PAIR),
            pl.ds(pl.multiple_of(D + p * PAIR, PAIR), PAIR),
        )

    def halo(block, step, sem, to):
        there = lax.rem(me + step + DEVICES, DEVICES)
        return pltpu.make_async_remote_copy(
            src_ref=cand.at[pl.ds(ROWS + block * BLOCK, BLOCK)],
            dst_ref=cand.at[pl.ds(to + block * BLOCK, BLOCK)],
            send_sem=halo_sems.at[sem], recv_sem=halo_sems.at[sem + 1],
            device_id=(there // 32, lax.rem(there, 32)), device_id_type=MESH,
        )

    node_tag = ones_where(iota((ROWS, PAIR), 1) == (iota((ROWS, PAIR), 0) >> 7))

    def encode_pairs(g, carry):
        spots = [pair_at(4 * g + i) for i in range(4)]
        outs = attend_pairs(
            [
                (query[:, at], node_tag, keyval[:, at], key_tags[...], keyval[:, upper])
                for at, upper in spots
            ]
        )
        for (at, _), out in zip(spots, outs):
            rows_a[:, at] = out
        return carry

    lax.fori_loop(0, 2, encode_pairs, 0)
    halos = []
    loads[5].wait()
    for block in range(2):
        here = pl.ds(block * BLOCK, BLOCK)

        def store_mid(at, out):
            mid[here, at] = (mesh[here, at].astype(F32) + out).astype(BF)

        project(rows_a.at[here], eo, D, 0, store_mid)
        norm_into(mid, block * BLOCK, cand, ROWS + block * BLOCK, process_gain, BLOCK)
        for step, sem, to in ((1, 4 * block, 0), (-1, 4 * block + 2, 2 * ROWS)):
            halos.append(halo(block, step, sem, to))
            halos[-1].start()
    for group in range(4):
        send_planes(
            send2, recv2, 2, 3 + group, group // 2, group % 2 * 2, group % 2 * 2 + 2, 1
        )

    loads[6].wait()

    def store_process_query(at, out):
        query[:, at] = (out * SCORE_SCALE).astype(BF)

    def store_own(at, out):
        keyval[pl.ds(0, ROWS), at] = out.astype(BF)

    def store_other(at, out):
        keyval[pl.ds(ROWS, ROWS), at] = out.astype(BF)

    own = cand.at[pl.ds(ROWS, ROWS)]
    project(own, pqkv, D, 0, store_process_query)
    project(own, pqkv, 2 * D, D, store_own)
    for copy in halos:
        copy.wait()
    for block in range(2):
        target = jnp.sum(
            jnp.where(iota((1, 2), 1) == block, neighbour_block[...], 0).astype(F32),
            axis=1,
            keepdims=True,
        )
        position = target - (2 * me - 2).astype(F32) + jnp.zeros((1, PAIR), F32)
        picked = None
        for candidate in (block, block + 1, block + 3, block + 4):
            weight = jnp.concatenate([ones_where(position == candidate)] * (D // PAIR), axis=1)
            term = cand[pl.ds(candidate * BLOCK, BLOCK), :] * weight
            picked = term if picked is None else picked + term
        rows_b[pl.ds(block * BLOCK, BLOCK), :] = picked
    project(rows_b, pqkv, 2 * D, D, store_other)

    def process_pairs(g, carry):
        spots = [(block, *pair_at(4 * g + i)) for i in range(4) for block in range(2)]
        work = []
        for block, at, upper in spots:
            here = pl.ds(block * BLOCK, BLOCK)
            there = pl.ds(ROWS + block * BLOCK, BLOCK)
            work.append(
                (
                    query[here, at], None,
                    jnp.concatenate([keyval[here, at], keyval[there, at]], axis=0), None,
                    jnp.concatenate([keyval[here, upper], keyval[there, upper]], axis=0),
                )
            )
        for (block, at, _), out in zip(spots, attend_pairs(work)):
            rows_a[pl.ds(block * BLOCK, BLOCK), at] = out
        return carry

    lax.fori_loop(0, 2, process_pairs, 0)
    loads[7].wait()

    def store_mesh_out(at, out):
        rows_b[:, at] = (mid[:, at].astype(F32) + out).astype(BF)

    project(rows_a, po, D, 0, store_mesh_out)
    norm_into(rows_b, 0, rows_a, 0, decode_mesh_gain)
    loads[8].wait()
    project(rows_a, dkv, 2 * D, 0, store_own)

    mine = pl.ds(0, ROWS)
    for chunk in range(4):
        here = pl.ds(chunk * BLOCK, BLOCK)
        wait_for(recv2, 32 * chunk, 32 * chunk + 32, recv_sems.at[3 + chunk])
        unpack(recv2, wide_rows, unmix, 2 * chunk, 2 * chunk + 2)

        spots = [pair_at(i) for i in range(8)]
        outs = attend_pairs(
            [
                (
                    wide_rows[here, at], query_tags[here, :],
                    keyval[mine, at], node_tag, keyval[mine, upper],
                )
                for at, upper in spots
            ]
        )
        for (at, _), out in zip(spots, outs):
            rows_a[pl.ds(0, BLOCK), at] = out
        for j in range(2):
            store_slabs(send3, 2 * chunk + j, rows_a[pl.ds(64 * j, 64), :], mix)
        send_planes(send3, recv3, 3, 7 + chunk, chunk // 2, chunk % 2 * 2, chunk % 2 * 2 + 2, -1)
    recv3[0] = send3[0]
    slot_column = jnp.sum(
        jnp.where(iota((ROWS, ROWS), 0) == iota((ROWS, ROWS), 1), d_slot, 0).astype(F32),
        axis=1,
        keepdims=True,
    )
    wait_for(send1, 0, DEVICES, send_sems.at[0])
    wait_for(lab_send, 0, DEVICES, send_sems.at[1])
    wait_for(send2, 0, DEVICES, send_sems.at[2])
    decoded = None
    for chunk in range(4):
        choose = ones_where(
            (iota((ROWS, BLOCK), 1) + chunk * BLOCK).astype(F32) == slot_column
        )
        wait_for(recv3, 32 * chunk, 32 * chunk + 32, recv_sems.at[7 + chunk])
        unpack(recv3, wide_rows, unmix, 2 * chunk, 2 * chunk + 2)
        found = matmul(choose, wide_rows[pl.ds(chunk * BLOCK, BLOCK), :])
        decoded = found if decoded is None else decoded + found
    rows_b[...] = decoded.astype(BF)
    loads[9].wait()

    def store_out(at, out):
        out_ref[:, at] = out.astype(BF)

    project(rows_b, do, D, 0, store_out)
    wait_for(send3, 0, DEVICES, send_sems.at[3])


def on_device(
    grid_state, mesh_state, encode_block, neighbour_block, decode_block,
    encode_grid_gain, encode_mesh_gain, process_gain, decode_grid_gain, decode_mesh_gain,
    encode_query, encode_keyval, encode_out, process_qkv, process_out,
    decode_query, decode_keyval, decode_out,
):
    hbm = pl.BlockSpec(memory_space=pl.ANY)
    vmem = pl.BlockSpec(memory_space=pltpu.VMEM)
    slabs = pltpu.VMEM((DEVICES, 16, 256), BF)
    rows = pltpu.VMEM((ROWS, D), BF)
    return pl.pallas_call(
        kernel,
        out_shape=jax.ShapeDtypeStruct((ROWS, D), BF),
        in_specs=[hbm, hbm, vmem, vmem, vmem] + [vmem] * 5 + [hbm] * 8,
        out_specs=vmem,
        scratch_shapes=[
            rows, rows,
            pltpu.VMEM((D, D), BF), pltpu.VMEM((D, 2 * D), BF), pltpu.VMEM((D, D), BF),
            pltpu.VMEM((D, 3 * D), BF), pltpu.VMEM((D, D), BF), pltpu.VMEM((D, D), BF),
            pltpu.VMEM((D, 2 * D), BF), pltpu.VMEM((D, D), BF),
            slabs, slabs, slabs, slabs, slabs, slabs,
            pltpu.VMEM((DEVICES, PAIR), F32),
            pltpu.VMEM((DEVICES, 1, PAIR), F32), pltpu.VMEM((DEVICES, 1, PAIR), F32),
            rows, rows, rows, rows,
            pltpu.VMEM((3 * ROWS, D), BF), pltpu.VMEM((SLOTS, D), BF),
            pltpu.VMEM((SLOTS, 2 * D), BF),
            pltpu.VMEM((SLOTS, PAIR), BF), pltpu.VMEM((SLOTS, PAIR), BF),
            pltpu.SemaphoreType.DMA((10,)), pltpu.SemaphoreType.DMA((4,)),
            pltpu.SemaphoreType.DMA((11,)), pltpu.SemaphoreType.DMA((8,)),
        ],
        compiler_params=pltpu.CompilerParams(
            collective_id=0, has_side_effects=True, vmem_limit_bytes=60 * 1024 * 1024
        ),
    )(
        grid_state, mesh_state, encode_block.reshape(1, -1), decode_block.reshape(1, -1),
        neighbour_block.reshape(1, -1),
        *(
            gain.reshape(1, -1)
            for gain in (
                encode_grid_gain, encode_mesh_gain, process_gain, decode_grid_gain, decode_mesh_gain,
            )
        ),
        encode_query, encode_keyval, encode_out, process_qkv, process_out,
        decode_query, decode_keyval, decode_out,
    )


def solution(mesh):
    rows, split = P(("gx", "gy"), None), P(("gx", "gy"))
    return jax.shard_map(
        on_device,
        mesh=mesh,
        in_specs=(rows, rows, split, split, split) + (P(),) * 13,
        out_specs=rows,
        check_vma=False,
    )
```

```python
import math

import jax
import jax.numpy as jnp
from jax import lax
from jax.experimental import pallas as pl
from jax.experimental.pallas import tpu as pltpu
from jax.sharding import PartitionSpec as P

HEADS = 16
BLOCK = 128
CAP = 4
DEVICES = 128
D = 1024
ROWS = 256
SLOTS = DEVICES * CAP
PAIR = 128
MASKED = -1e30
SCORE_SCALE = 0.125 * math.log2(math.e)
MESH = pl.DeviceIdType.MESH
BF = jnp.bfloat16
F32 = jnp.float32


def coordinates():
    gy = lax.axis_index("gy")
    return lax.axis_index("gx"), gy // 8, lax.rem(gy // 2, 4), lax.rem(gy, 2)


def each_peer(visit, core, first, last, sign):
    z, x, y, c = coordinates()
    columns = [lax.rem(x + i, 4) * 8 for i in range(4)]
    lines = [lax.rem(y + i, 4) * 2 for i in range(4)]
    side = c if core == 0 else 1 - c

    def plane(kz, start):
        gx = lax.rem(z + sign * kz + 4, 4)
        for ky in range(4):
            line = lines[sign * ky % 4] + side
            for kx in range(4):
                if kx + 4 * ky >= start:
                    visit(64 * core + 16 * kz + 4 * ky + kx, (gx, columns[sign * kx % 4] + line))

    if core == 0 and first == 0:
        plane(0, 1)
        first = 1

    def step(kz, carry):
        plane(kz, 0)
        return carry

    lax.fori_loop(first, last, step, 0)


def iota(shape, dim):
    return lax.broadcasted_iota(jnp.int32, shape, dim)


def ones_where(condition, dtype=BF):
    return jnp.where(condition, 1.0, 0.0).astype(dtype)


def matmul(a, b):
    return jnp.dot(a, b, preferred_element_type=F32)


def matmul_nt(a, b):
    return lax.dot_general(a, b, (((1,), (1,)), ((), ())), preferred_element_type=F32)


def norm_into(src, src_row, dst, dst_row, gain_ref, rows=ROWS):
    def step(i, carry):
        wide = src[pl.ds(pl.multiple_of(src_row + i * 32, 32), 32), :].astype(F32)
        scale = lax.rsqrt(jnp.mean(wide * wide, axis=-1, keepdims=True) + 1e-6)
        dst[pl.ds(pl.multiple_of(dst_row + i * 32, 32), 32), :] = (
            wide * scale * gain_ref[...]
        ).astype(BF)
        return carry

    lax.fori_loop(0, rows // 32, step, 0)


def project(a_ref, w_ref, columns, first_column, epilogue, tile=512):
    def step(n, carry):
        at = pl.multiple_of(n * tile, tile)
        out = matmul(a_ref[...], w_ref[:, pl.ds(pl.multiple_of(first_column + at, tile), tile)])
        epilogue(pl.ds(at, tile), out)
        return carry

    lax.fori_loop(0, columns // tile, step, 0, unroll=True)


def slot_plan(blocks):
    z, x, y, c = coordinates()
    owner = blocks >> 1
    k = (
        (((owner >> 3) & 3) - x & 3)
        + 4 * (((owner >> 1) & 3) - y & 3)
        + 16 * ((owner >> 5) - z & 3)
        + 64 * ((owner & 1) - c & 1)
    )
    matches = ones_where(iota((DEVICES, ROWS), 0) == k)
    earlier = ones_where(iota((ROWS, ROWS), 0) < iota((ROWS, ROWS), 1))
    counts = matmul(matches, earlier)
    rank = jnp.sum(matches.astype(F32) * counts, axis=0, keepdims=True).astype(jnp.int32)
    return matches, rank, k * CAP + rank


def label_table(matches, rank, blocks, base):
    coded = jnp.where(iota((PAIR, ROWS), 0) == rank + base, (blocks & 1) + 1, 0)
    return matmul_nt(matches, coded.astype(F32).astype(BF))


def interleave():
    m = iota((256, 256), 0)
    return ones_where(iota((256, 256), 1) == 64 * ((m >> 2) & 3) + 4 * (m >> 4) + (m & 3))


def separate():
    n = iota((256, 256), 0)
    return ones_where(iota((256, 256), 1) == 16 * ((n >> 2) & 15) + 4 * (n >> 6) + (n & 3))


def store_slabs(dst, j, rows, mix):
    tall = jnp.concatenate([rows[:, 256 * q : 256 * q + 256] for q in range(4)], axis=0)
    dst[pl.ds(16 * j, 16)] = matmul(mix, tall).astype(BF).reshape(16, 16, 256)


def load_slabs(src, j, unmix):
    tall = matmul(unmix, src[pl.ds(16 * j, 16)].reshape(256, 256)).astype(BF)
    return jnp.concatenate([tall[64 * q : 64 * q + 64] for q in range(4)], axis=1)


def pack(rows_ref, slot, dst, mix, half):
    chosen = ones_where(iota((ROWS, ROWS), 0) + ROWS * half == slot)
    rows = matmul(chosen, rows_ref[...]).astype(BF)
    for j in range(4):
        store_slabs(dst, 4 * half + j, rows[64 * j : 64 * j + 64], mix)


def unpack(src, dst, unmix, first, last):
    def step(j, carry):
        dst[pl.ds(pl.multiple_of(64 * j, 64), 64), :] = load_slabs(src, j, unmix)
        return carry

    lax.fori_loop(first, last, step, 0, unroll=True)


def attend_pairs(pairs):
    lane = iota((1, PAIR), 1)
    scores, outs = [], []
    for queries, query_tag, keys, key_tag, values in pairs:
        if key_tag is not None:
            keys = jnp.concatenate([keys, key_tag], axis=1)
        for half in range(2):
            part = queries * ones_where((lane >= 64) == (half == 1))
            if query_tag is not None:
                part = jnp.concatenate([part, query_tag], axis=1)
            scores.append(matmul_nt(part, keys))
    powers = [jnp.exp2(x - jnp.max(x, axis=-1, keepdims=True)).astype(BF) for x in scores]
    for i, (_, _, _, _, values) in enumerate(pairs):
        widened = jnp.concatenate([values, jnp.ones_like(values)], axis=1)
        halves = [matmul(powers[2 * i + half], widened) for half in range(2)]
        halves = [both[:, :PAIR] / both[:, PAIR:] for both in halves]
        outs.append(jnp.where(lane < 64, halves[0], halves[1]).astype(BF))
    return outs


def kernel(
    grid_hbm, mesh_hbm, encode_block, decode_block, neighbour_block,
    encode_grid_gain, encode_mesh_gain, process_gain, decode_grid_gain, decode_mesh_gain,
    eq_hbm, ekv_hbm, eo_hbm, pqkv_hbm, po_hbm, dq_hbm, dkv_hbm, do_hbm,
    out_ref,
    grid, mesh, eq, ekv, eo, pqkv, po, dq, dkv, do,
    send1, recv1, send2, recv2, send3, recv3, lab2d, lab_send, lab_recv,
    rows_a, rows_b, query, mid, cand, wide_rows, keyval, key_tags, query_tags,
    load_sems, send_sems, recv_sems, halo_sems,
):
    z, x, y, c = coordinates()
    me = lax.axis_index("gx") * 32 + lax.axis_index("gy")
    barrier = pltpu.get_barrier_semaphore()

    def greet(k, device):
        pl.semaphore_signal(barrier, inc=1, device_id=device, device_id_type=MESH)

    loads = [
        pltpu.make_async_copy(src, dst, load_sems.at[i])
        for i, (src, dst) in enumerate(
            (
                (grid_hbm, grid), (dq_hbm, dq), (mesh_hbm, mesh), (eq_hbm, eq), (ekv_hbm, ekv),
                (eo_hbm, eo), (pqkv_hbm, pqkv), (po_hbm, po), (dkv_hbm, dkv), (do_hbm, do),
            )
        )
    ]
    loads[0].start()
    each_peer(greet, 0, 0, 4, 1)
    each_peer(greet, 1, 0, 4, 1)
    for load in loads[1:]:
        load.start()

    def send_planes(src, dst, sent, received, core, first, last, sign):
        def send(k, device):
            pltpu.make_async_remote_copy(
                src_ref=src.at[k], dst_ref=dst.at[k], send_sem=send_sems.at[sent],
                recv_sem=recv_sems.at[received], device_id=device, device_id_type=MESH,
            ).start()

        each_peer(send, core, first, last, sign)

    def wait_for(ref, first, last, sem):
        view = ref.at[pl.ds(max(1, first), last - max(1, first))]
        pltpu.make_async_copy(view, view, sem).wait()

    mix, unmix = interleave(), separate()
    e_matches, e_rank, e_slot = slot_plan(encode_block[...])
    loads[0].wait()
    norm_into(grid, 0, rows_a, 0, encode_grid_gain)
    pack(rows_a, e_slot, send1, mix, 0)
    pl.semaphore_wait(barrier, DEVICES - 1)
    send_planes(send1, recv1, 0, 0, 0, 0, 4, 1)
    d_matches, d_rank, d_slot = slot_plan(decode_block[...])
    lab2d[...] = label_table(e_matches, e_rank, encode_block[...], 0) + label_table(
        d_matches, d_rank, decode_block[...], CAP
    )

    def spread(k, carry):
        lab_send[k] = lab2d[pl.ds(k, 1), :]
        return carry

    lax.fori_loop(0, DEVICES, spread, 0, unroll=8)
    for core in range(2):
        send_planes(lab_send, lab_recv, 1, 2, core, 0, 4, 1)
    pack(rows_a, e_slot, send1, mix, 1)
    send_planes(send1, recv1, 0, 1, 1, 0, 4, 1)

    norm_into(grid, 0, rows_a, 0, decode_grid_gain)

    loads[1].wait()

    def store_query(at, out):
        rows_b[:, at] = (out * SCORE_SCALE).astype(BF)

    project(rows_a, dq, D, 0, store_query)
    pack(rows_b, d_slot, send2, mix, 0)
    for group in range(2):
        send_planes(send2, recv2, 2, 3 + group, 0, 2 * group, 2 * group + 2, 1)
    pack(rows_b, d_slot, send2, mix, 1)

    loads[2].wait()
    norm_into(mesh, 0, rows_a, 0, encode_mesh_gain)
    loads[3].wait()

    def store_mesh_query(at, out):
        query[:, at] = (out * SCORE_SCALE).astype(BF)

    project(rows_a, eq, D, 0, store_mesh_query)
    recv1[0] = send1[0]
    recv2[0] = send2[0]
    lab_recv[0] = lab_send[0]
    loads[4].wait()
    def key_values(group):
        wait_for(recv1, 64 * group, 64 * group + 64, recv_sems.at[group])
        unpack(recv1, wide_rows, unmix, 4 * group, 4 * group + 4)
        part = pl.ds(group * ROWS, ROWS)

        def store_keyval(at, out):
            keyval[part, at] = out.astype(BF)

        project(wide_rows.at[part], ekv, 2 * D, 0, store_keyval)

    key_values(0)
    wait_for(lab_recv, 0, DEVICES, recv_sems.at[2])

    def gather_labels(k, carry):
        lab2d[pl.ds(k, 1), :] = lab_recv[k]
        return carry

    lax.fori_loop(0, DEVICES, gather_labels, 0, unroll=8)
    spread_rows = matmul(
        ones_where((iota((SLOTS, DEVICES), 0) >> 2) == iota((SLOTS, DEVICES), 1)),
        lab2d[...].astype(BF),
    )
    slot_lane = iota((SLOTS, PAIR), 1)
    slot_rank = iota((SLOTS, PAIR), 0) & 3

    def slot_tags(base):
        label = jnp.sum(
            jnp.where(slot_lane == base + slot_rank, spread_rows, 0.0), axis=1, keepdims=True
        )
        other = label != (slot_lane + 1).astype(F32)
        return jnp.where(other & (slot_lane < 2), MASKED, 0.0).astype(BF)

    key_tags[...] = slot_tags(0)
    query_tags[...] = slot_tags(CAP)

    key_values(1)

    def pair_at(p):
        if isinstance(p, int):
            return pl.ds(p * PAIR, PAIR), pl.ds(D + p * PAIR, PAIR)
        return (
            pl.ds(pl.multiple_of(p * PAIR, PAIR), PAIR),
            pl.ds(pl.multiple_of(D + p * PAIR, PAIR), PAIR),
        )

    def halo(block, step, sem, to):
        there = lax.rem(me + step + DEVICES, DEVICES)
        return pltpu.make_async_remote_copy(
            src_ref=cand.at[pl.ds(ROWS + block * BLOCK, BLOCK)],
            dst_ref=cand.at[pl.ds(to + block * BLOCK, BLOCK)],
            send_sem=halo_sems.at[sem], recv_sem=halo_sems.at[sem + 1],
            device_id=(there // 32, lax.rem(there, 32)), device_id_type=MESH,
        )

    node_tag = ones_where(iota((ROWS, PAIR), 1) == (iota((ROWS, PAIR), 0) >> 7))

    def encode_pairs(g, carry):
        spots = [pair_at(4 * g + i) for i in range(4)]
        outs = attend_pairs(
            [
                (query[:, at], node_tag, keyval[:, at], key_tags[...], keyval[:, upper])
                for at, upper in spots
            ]
        )
        for (at, _), out in zip(spots, outs):
            rows_a[:, at] = out
        return carry

    lax.fori_loop(0, 2, encode_pairs, 0)
    halos = []
    loads[5].wait()
    for block in range(2):
        here = pl.ds(block * BLOCK, BLOCK)

        def store_mid(at, out):
            mid[here, at] = (mesh[here, at].astype(F32) + out).astype(BF)

        project(rows_a.at[here], eo, D, 0, store_mid)
        norm_into(mid, block * BLOCK, cand, ROWS + block * BLOCK, process_gain, BLOCK)
        for step, sem, to in ((1, 4 * block, 0), (-1, 4 * block + 2, 2 * ROWS)):
            halos.append(halo(block, step, sem, to))
            halos[-1].start()
    for group in range(2):
        send_planes(send2, recv2, 2, 5 + group, 1, 2 * group, 2 * group + 2, 1)

    loads[6].wait()

    def store_process_query(at, out):
        query[:, at] = (out * SCORE_SCALE).astype(BF)

    def store_own(at, out):
        keyval[pl.ds(0, ROWS), at] = out.astype(BF)

    def store_other(at, out):
        keyval[pl.ds(ROWS, ROWS), at] = out.astype(BF)

    own = cand.at[pl.ds(ROWS, ROWS)]
    project(own, pqkv, D, 0, store_process_query)
    project(own, pqkv, 2 * D, D, store_own)
    for copy in halos:
        copy.wait()
    for block in range(2):
        target = jnp.sum(
            jnp.where(iota((1, 2), 1) == block, neighbour_block[...], 0).astype(F32),
            axis=1,
            keepdims=True,
        )
        position = target - (2 * me - 2).astype(F32) + jnp.zeros((1, PAIR), F32)
        picked = None
        for candidate in (block, block + 1, block + 3, block + 4):
            weight = jnp.concatenate([ones_where(position == candidate)] * (D // PAIR), axis=1)
            term = cand[pl.ds(candidate * BLOCK, BLOCK), :] * weight
            picked = term if picked is None else picked + term
        rows_b[pl.ds(block * BLOCK, BLOCK), :] = picked
    project(rows_b, pqkv, 2 * D, D, store_other)

    def process_pairs(g, carry):
        spots = [(block, *pair_at(4 * g + i)) for i in range(4) for block in range(2)]
        work = []
        for block, at, upper in spots:
            here = pl.ds(block * BLOCK, BLOCK)
            there = pl.ds(ROWS + block * BLOCK, BLOCK)
            work.append(
                (
                    query[here, at], None,
                    jnp.concatenate([keyval[here, at], keyval[there, at]], axis=0), None,
                    jnp.concatenate([keyval[here, upper], keyval[there, upper]], axis=0),
                )
            )
        for (block, at, _), out in zip(spots, attend_pairs(work)):
            rows_a[pl.ds(block * BLOCK, BLOCK), at] = out
        return carry

    lax.fori_loop(0, 2, process_pairs, 0)
    loads[7].wait()

    def store_mesh_out(at, out):
        rows_b[:, at] = (mid[:, at].astype(F32) + out).astype(BF)

    project(rows_a, po, D, 0, store_mesh_out)
    norm_into(rows_b, 0, rows_a, 0, decode_mesh_gain)
    loads[8].wait()
    project(rows_a, dkv, 2 * D, 0, store_own)

    mine = pl.ds(0, ROWS)
    for chunk in range(4):
        here = pl.ds(chunk * BLOCK, BLOCK)
        wait_for(recv2, 32 * chunk, 32 * chunk + 32, recv_sems.at[3 + chunk])
        unpack(recv2, wide_rows, unmix, 2 * chunk, 2 * chunk + 2)

        spots = [pair_at(i) for i in range(8)]
        outs = attend_pairs(
            [
                (
                    wide_rows[here, at], query_tags[here, :],
                    keyval[mine, at], node_tag, keyval[mine, upper],
                )
                for at, upper in spots
            ]
        )
        for (at, _), out in zip(spots, outs):
            rows_a[pl.ds(0, BLOCK), at] = out
        for j in range(2):
            store_slabs(send3, 2 * chunk + j, rows_a[pl.ds(64 * j, 64), :], mix)
        send_planes(send3, recv3, 3, 7 + chunk, chunk // 2, chunk % 2 * 2, chunk % 2 * 2 + 2, -1)
    recv3[0] = send3[0]
    slot_column = jnp.sum(
        jnp.where(iota((ROWS, ROWS), 0) == iota((ROWS, ROWS), 1), d_slot, 0).astype(F32),
        axis=1,
        keepdims=True,
    )
    wait_for(send1, 0, DEVICES, send_sems.at[0])
    wait_for(lab_send, 0, DEVICES, send_sems.at[1])
    wait_for(send2, 0, DEVICES, send_sems.at[2])
    decoded = None
    for chunk in range(4):
        choose = ones_where(
            (iota((ROWS, BLOCK), 1) + chunk * BLOCK).astype(F32) == slot_column
        )
        wait_for(recv3, 32 * chunk, 32 * chunk + 32, recv_sems.at[7 + chunk])
        unpack(recv3, wide_rows, unmix, 2 * chunk, 2 * chunk + 2)
        found = matmul(choose, wide_rows[pl.ds(chunk * BLOCK, BLOCK), :])
        decoded = found if decoded is None else decoded + found
    rows_b[...] = decoded.astype(BF)
    loads[9].wait()

    def store_out(at, out):
        out_ref[:, at] = out.astype(BF)

    project(rows_b, do, D, 0, store_out)
    wait_for(send3, 0, DEVICES, send_sems.at[3])


def on_device(
    grid_state, mesh_state, encode_block, neighbour_block, decode_block,
    encode_grid_gain, encode_mesh_gain, process_gain, decode_grid_gain, decode_mesh_gain,
    encode_query, encode_keyval, encode_out, process_qkv, process_out,
    decode_query, decode_keyval, decode_out,
):
    hbm = pl.BlockSpec(memory_space=pl.ANY)
    vmem = pl.BlockSpec(memory_space=pltpu.VMEM)
    slabs = pltpu.VMEM((DEVICES, 16, 256), BF)
    rows = pltpu.VMEM((ROWS, D), BF)
    return pl.pallas_call(
        kernel,
        out_shape=jax.ShapeDtypeStruct((ROWS, D), BF),
        in_specs=[hbm, hbm, vmem, vmem, vmem] + [vmem] * 5 + [hbm] * 8,
        out_specs=vmem,
        scratch_shapes=[
            rows, rows,
            pltpu.VMEM((D, D), BF), pltpu.VMEM((D, 2 * D), BF), pltpu.VMEM((D, D), BF),
            pltpu.VMEM((D, 3 * D), BF), pltpu.VMEM((D, D), BF), pltpu.VMEM((D, D), BF),
            pltpu.VMEM((D, 2 * D), BF), pltpu.VMEM((D, D), BF),
            slabs, slabs, slabs, slabs, slabs, slabs,
            pltpu.VMEM((DEVICES, PAIR), F32),
            pltpu.VMEM((DEVICES, 1, PAIR), F32), pltpu.VMEM((DEVICES, 1, PAIR), F32),
            rows, rows, rows, rows,
            pltpu.VMEM((3 * ROWS, D), BF), pltpu.VMEM((SLOTS, D), BF),
            pltpu.VMEM((SLOTS, 2 * D), BF),
            pltpu.VMEM((SLOTS, PAIR), BF), pltpu.VMEM((SLOTS, PAIR), BF),
            pltpu.SemaphoreType.DMA((10,)), pltpu.SemaphoreType.DMA((4,)),
            pltpu.SemaphoreType.DMA((11,)), pltpu.SemaphoreType.DMA((8,)),
        ],
        compiler_params=pltpu.CompilerParams(
            collective_id=0, has_side_effects=True, vmem_limit_bytes=60 * 1024 * 1024
        ),
    )(
        grid_state, mesh_state, encode_block.reshape(1, -1), decode_block.reshape(1, -1),
        neighbour_block.reshape(1, -1),
        *(
            gain.reshape(1, -1)
            for gain in (
                encode_grid_gain, encode_mesh_gain, process_gain, decode_grid_gain, decode_mesh_gain,
            )
        ),
        encode_query, encode_keyval, encode_out, process_qkv, process_out,
        decode_query, decode_keyval, decode_out,
    )


def solution(mesh):
    rows, split = P(("gx", "gy"), None), P(("gx", "gy"))
    return jax.shard_map(
        on_device,
        mesh=mesh,
        in_specs=(rows, rows, split, split, split) + (P(),) * 13,
        out_specs=rows,
        check_vma=False,
    )
```

```python
import math

import jax
import jax.numpy as jnp
from jax import lax
from jax.experimental import pallas as pl
from jax.experimental.pallas import tpu as pltpu
from jax.sharding import PartitionSpec as P

HEADS = 16
BLOCK = 128
CAP = 4
DEVICES = 128
D = 1024
ROWS = 256
SLOTS = DEVICES * CAP
PAIR = 128
MASKED = -1e30
SCORE_SCALE = 0.125 * math.log2(math.e)
MESH = pl.DeviceIdType.MESH
BF = jnp.bfloat16
F32 = jnp.float32


def coordinates():
    gy = lax.axis_index("gy")
    return lax.axis_index("gx"), gy // 8, lax.rem(gy // 2, 4), lax.rem(gy, 2)


def each_peer(visit, core, first, last, sign):
    z, x, y, c = coordinates()
    columns = [lax.rem(x + i, 4) * 8 for i in range(4)]
    lines = [lax.rem(y + i, 4) * 2 for i in range(4)]
    side = c if core == 0 else 1 - c

    def plane(kz, start):
        gx = lax.rem(z + sign * kz + 4, 4)
        for ky in range(4):
            line = lines[sign * ky % 4] + side
            for kx in range(4):
                if kx + 4 * ky >= start:
                    visit(64 * core + 16 * kz + 4 * ky + kx, (gx, columns[sign * kx % 4] + line))

    if core == 0 and first == 0:
        plane(0, 1)
        first = 1

    def step(kz, carry):
        plane(kz, 0)
        return carry

    lax.fori_loop(first, last, step, 0)


def iota(shape, dim):
    return lax.broadcasted_iota(jnp.int32, shape, dim)


def ones_where(condition, dtype=BF):
    return jnp.where(condition, 1.0, 0.0).astype(dtype)


def matmul(a, b):
    return jnp.dot(a, b, preferred_element_type=F32)


def matmul_nt(a, b):
    return lax.dot_general(a, b, (((1,), (1,)), ((), ())), preferred_element_type=F32)


def norm_into(src, src_row, dst, dst_row, gain_ref, rows=ROWS):
    def step(i, carry):
        wide = src[pl.ds(pl.multiple_of(src_row + i * 32, 32), 32), :].astype(F32)
        scale = lax.rsqrt(jnp.mean(wide * wide, axis=-1, keepdims=True) + 1e-6)
        dst[pl.ds(pl.multiple_of(dst_row + i * 32, 32), 32), :] = (
            wide * scale * gain_ref[...]
        ).astype(BF)
        return carry

    lax.fori_loop(0, rows // 32, step, 0)


def project(a_ref, w_ref, columns, first_column, epilogue, tile=512):
    def step(n, carry):
        at = pl.multiple_of(n * tile, tile)
        out = matmul(a_ref[...], w_ref[:, pl.ds(pl.multiple_of(first_column + at, tile), tile)])
        epilogue(pl.ds(at, tile), out)
        return carry

    lax.fori_loop(0, columns // tile, step, 0, unroll=True)


def slot_plan(blocks):
    z, x, y, c = coordinates()
    owner = blocks >> 1
    k = (
        (((owner >> 3) & 3) - x & 3)
        + 4 * (((owner >> 1) & 3) - y & 3)
        + 16 * ((owner >> 5) - z & 3)
        + 64 * ((owner & 1) - c & 1)
    )
    matches = ones_where(iota((DEVICES, ROWS), 0) == k)
    earlier = ones_where(iota((ROWS, ROWS), 0) < iota((ROWS, ROWS), 1))
    counts = matmul(matches, earlier)
    rank = jnp.sum(matches.astype(F32) * counts, axis=0, keepdims=True).astype(jnp.int32)
    return matches, rank, k * CAP + rank


def label_table(matches, rank, blocks, base):
    coded = jnp.where(iota((PAIR, ROWS), 0) == rank + base, (blocks & 1) + 1, 0)
    return matmul_nt(matches, coded.astype(F32).astype(BF))


def interleave():
    m = iota((256, 256), 0)
    return ones_where(iota((256, 256), 1) == 64 * ((m >> 2) & 3) + 4 * (m >> 4) + (m & 3))


def separate():
    n = iota((256, 256), 0)
    return ones_where(iota((256, 256), 1) == 16 * ((n >> 2) & 15) + 4 * (n >> 6) + (n & 3))


def store_slabs(dst, j, rows, mix):
    tall = jnp.concatenate([rows[:, 256 * q : 256 * q + 256] for q in range(4)], axis=0)
    dst[pl.ds(16 * j, 16)] = matmul(mix, tall).astype(BF).reshape(16, 16, 256)


def load_slabs(src, j, unmix):
    tall = matmul(unmix, src[pl.ds(16 * j, 16)].reshape(256, 256)).astype(BF)
    return jnp.concatenate([tall[64 * q : 64 * q + 64] for q in range(4)], axis=1)


def pack(rows_ref, slot, dst, mix, half):
    chosen = ones_where(iota((ROWS, ROWS), 0) + ROWS * half == slot)
    rows = matmul(chosen, rows_ref[...]).astype(BF)
    for j in range(4):
        store_slabs(dst, 4 * half + j, rows[64 * j : 64 * j + 64], mix)


def unpack(src, dst, unmix, first, last):
    def step(j, carry):
        dst[pl.ds(pl.multiple_of(64 * j, 64), 64), :] = load_slabs(src, j, unmix)
        return carry

    lax.fori_loop(first, last, step, 0, unroll=True)


def attend_pairs(pairs):
    lane = iota((1, PAIR), 1)
    scores, outs = [], []
    for queries, query_tag, keys, key_tag, values in pairs:
        if key_tag is not None:
            keys = jnp.concatenate([keys, key_tag], axis=1)
        for half in range(2):
            part = queries * ones_where((lane >= 64) == (half == 1))
            if query_tag is not None:
                part = jnp.concatenate([part, query_tag], axis=1)
            scores.append(matmul_nt(part, keys))
    powers = [jnp.exp2(x - jnp.max(x, axis=-1, keepdims=True)).astype(BF) for x in scores]
    for i, (_, _, _, _, values) in enumerate(pairs):
        widened = jnp.concatenate([values, jnp.ones_like(values)], axis=1)
        halves = [matmul(powers[2 * i + half], widened) for half in range(2)]
        halves = [both[:, :PAIR] / both[:, PAIR:] for both in halves]
        outs.append(jnp.where(lane < 64, halves[0], halves[1]).astype(BF))
    return outs


def kernel(
    grid_hbm, mesh_hbm, eb_hbm, db_hbm, nb_hbm, eg_hbm, em_hbm, pg_hbm, dg_hbm, dm_hbm, eq_hbm, ekv_hbm, eo_hbm, pqkv_hbm, po_hbm, dq_hbm, dkv_hbm, do_hbm,
    out_ref,
    encode_block, decode_block, neighbour_block,
    encode_grid_gain, encode_mesh_gain, process_gain, decode_grid_gain, decode_mesh_gain,
    grid, mesh, eq, ekv, eo, pqkv, po, dq, dkv, do,
    send1, recv1, send2, recv2, send3, recv3, lab2d, lab_send, lab_recv,
    rows_a, rows_b, query, mid, cand, wide_rows, keyval, key_tags, query_tags,
    load_sems, send_sems, recv_sems, halo_sems,
):
    z, x, y, c = coordinates()
    me = lax.axis_index("gx") * 32 + lax.axis_index("gy")
    barrier = pltpu.get_barrier_semaphore()

    def greet(k, device):
        pl.semaphore_signal(barrier, inc=1, device_id=device, device_id_type=MESH)

    loads = [
        pltpu.make_async_copy(src, dst, load_sems.at[i])
        for i, (src, dst) in enumerate(
            (
                (grid_hbm, grid), (dq_hbm, dq), (mesh_hbm, mesh), (eq_hbm, eq), (ekv_hbm, ekv),
                (eo_hbm, eo), (pqkv_hbm, pqkv), (po_hbm, po), (dkv_hbm, dkv), (do_hbm, do),
            )
        )
    ]
    small = [
        pltpu.make_async_copy(src, dst, load_sems.at[10 + i])
        for i, (src, dst) in enumerate(
            (
                (eb_hbm, encode_block), (db_hbm, decode_block), (nb_hbm, neighbour_block),
                (eg_hbm, encode_grid_gain), (em_hbm, encode_mesh_gain), (pg_hbm, process_gain),
                (dg_hbm, decode_grid_gain), (dm_hbm, decode_mesh_gain),
            )
        )
    ]
    loads[0].start()
    for load in small:
        load.start()
    each_peer(greet, 0, 0, 4, 1)
    each_peer(greet, 1, 0, 4, 1)
    for load in loads[1:]:
        load.start()

    def send_planes(src, dst, sent, received, core, first, last, sign):
        def send(k, device):
            pltpu.make_async_remote_copy(
                src_ref=src.at[k], dst_ref=dst.at[k], send_sem=send_sems.at[sent],
                recv_sem=recv_sems.at[received], device_id=device, device_id_type=MESH,
            ).start()

        each_peer(send, core, first, last, sign)

    def wait_for(ref, first, last, sem):
        view = ref.at[pl.ds(max(1, first), last - max(1, first))]
        pltpu.make_async_copy(view, view, sem).wait()

    mix, unmix = interleave(), separate()
    for load in small:
        load.wait()
    e_matches, e_rank, e_slot = slot_plan(encode_block[...])
    loads[0].wait()
    norm_into(grid, 0, rows_a, 0, encode_grid_gain)
    pack(rows_a, e_slot, send1, mix, 0)
    pl.semaphore_wait(barrier, DEVICES - 1)
    send_planes(send1, recv1, 0, 0, 0, 0, 4, 1)
    d_matches, d_rank, d_slot = slot_plan(decode_block[...])
    lab2d[...] = label_table(e_matches, e_rank, encode_block[...], 0) + label_table(
        d_matches, d_rank, decode_block[...], CAP
    )

    def spread(k, carry):
        lab_send[k] = lab2d[pl.ds(k, 1), :]
        return carry

    lax.fori_loop(0, DEVICES, spread, 0, unroll=8)
    for core in range(2):
        send_planes(lab_send, lab_recv, 1, 2, core, 0, 4, 1)
    pack(rows_a, e_slot, send1, mix, 1)
    send_planes(send1, recv1, 0, 1, 1, 0, 4, 1)

    norm_into(grid, 0, rows_a, 0, decode_grid_gain)

    loads[1].wait()

    def store_query(at, out):
        rows_b[:, at] = (out * SCORE_SCALE).astype(BF)

    project(rows_a, dq, D, 0, store_query)
    pack(rows_b, d_slot, send2, mix, 0)
    for group in range(2):
        send_planes(send2, recv2, 2, 3 + group, 0, 2 * group, 2 * group + 2, 1)
    pack(rows_b, d_slot, send2, mix, 1)

    loads[2].wait()
    norm_into(mesh, 0, rows_a, 0, encode_mesh_gain)
    loads[3].wait()

    def store_mesh_query(at, out):
        query[:, at] = (out * SCORE_SCALE).astype(BF)

    project(rows_a, eq, D, 0, store_mesh_query)
    recv1[0] = send1[0]
    recv2[0] = send2[0]
    lab_recv[0] = lab_send[0]
    loads[4].wait()
    def key_values(group):
        wait_for(recv1, 64 * group, 64 * group + 64, recv_sems.at[group])
        unpack(recv1, wide_rows, unmix, 4 * group, 4 * group + 4)
        part = pl.ds(group * ROWS, ROWS)

        def store_keyval(at, out):
            keyval[part, at] = out.astype(BF)

        project(wide_rows.at[part], ekv, 2 * D, 0, store_keyval)

    key_values(0)
    wait_for(lab_recv, 0, DEVICES, recv_sems.at[2])

    def gather_labels(k, carry):
        lab2d[pl.ds(k, 1), :] = lab_recv[k]
        return carry

    lax.fori_loop(0, DEVICES, gather_labels, 0, unroll=8)
    spread_rows = matmul(
        ones_where((iota((SLOTS, DEVICES), 0) >> 2) == iota((SLOTS, DEVICES), 1)),
        lab2d[...].astype(BF),
    )
    slot_lane = iota((SLOTS, PAIR), 1)
    slot_rank = iota((SLOTS, PAIR), 0) & 3

    def slot_tags(base):
        label = jnp.sum(
            jnp.where(slot_lane == base + slot_rank, spread_rows, 0.0), axis=1, keepdims=True
        )
        other = label != (slot_lane + 1).astype(F32)
        return jnp.where(other & (slot_lane < 2), MASKED, 0.0).astype(BF)

    key_tags[...] = slot_tags(0)
    query_tags[...] = slot_tags(CAP)

    key_values(1)

    def pair_at(p):
        if isinstance(p, int):
            return pl.ds(p * PAIR, PAIR), pl.ds(D + p * PAIR, PAIR)
        return (
            pl.ds(pl.multiple_of(p * PAIR, PAIR), PAIR),
            pl.ds(pl.multiple_of(D + p * PAIR, PAIR), PAIR),
        )

    def halo(block, step, sem, to):
        there = lax.rem(me + step + DEVICES, DEVICES)
        return pltpu.make_async_remote_copy(
            src_ref=cand.at[pl.ds(ROWS + block * BLOCK, BLOCK)],
            dst_ref=cand.at[pl.ds(to + block * BLOCK, BLOCK)],
            send_sem=halo_sems.at[sem], recv_sem=halo_sems.at[sem + 1],
            device_id=(there // 32, lax.rem(there, 32)), device_id_type=MESH,
        )

    node_tag = ones_where(iota((ROWS, PAIR), 1) == (iota((ROWS, PAIR), 0) >> 7))

    def encode_pairs(g, carry):
        spots = [pair_at(4 * g + i) for i in range(4)]
        outs = attend_pairs(
            [
                (query[:, at], node_tag, keyval[:, at], key_tags[...], keyval[:, upper])
                for at, upper in spots
            ]
        )
        for (at, _), out in zip(spots, outs):
            rows_a[:, at] = out
        return carry

    lax.fori_loop(0, 2, encode_pairs, 0)
    halos = []
    loads[5].wait()
    for block in range(2):
        here = pl.ds(block * BLOCK, BLOCK)

        def store_mid(at, out):
            mid[here, at] = (mesh[here, at].astype(F32) + out).astype(BF)

        project(rows_a.at[here], eo, D, 0, store_mid)
        norm_into(mid, block * BLOCK, cand, ROWS + block * BLOCK, process_gain, BLOCK)
        for step, sem, to in ((1, 4 * block, 0), (-1, 4 * block + 2, 2 * ROWS)):
            halos.append(halo(block, step, sem, to))
            halos[-1].start()
    for group in range(2):
        send_planes(send2, recv2, 2, 5 + group, 1, 2 * group, 2 * group + 2, 1)

    loads[6].wait()

    def store_process_query(at, out):
        query[:, at] = (out * SCORE_SCALE).astype(BF)

    def store_own(at, out):
        keyval[pl.ds(0, ROWS), at] = out.astype(BF)

    def store_other(at, out):
        keyval[pl.ds(ROWS, ROWS), at] = out.astype(BF)

    own = cand.at[pl.ds(ROWS, ROWS)]
    project(own, pqkv, D, 0, store_process_query)
    project(own, pqkv, 2 * D, D, store_own)
    for copy in halos:
        copy.wait()
    for block in range(2):
        target = jnp.sum(
            jnp.where(iota((1, 2), 1) == block, neighbour_block[...], 0).astype(F32),
            axis=1,
            keepdims=True,
        )
        position = target - (2 * me - 2).astype(F32) + jnp.zeros((1, PAIR), F32)
        picked = None
        for candidate in (block, block + 1, block + 3, block + 4):
            weight = jnp.concatenate([ones_where(position == candidate)] * (D // PAIR), axis=1)
            term = cand[pl.ds(candidate * BLOCK, BLOCK), :] * weight
            picked = term if picked is None else picked + term
        rows_b[pl.ds(block * BLOCK, BLOCK), :] = picked
    project(rows_b, pqkv, 2 * D, D, store_other)

    def process_pairs(g, carry):
        spots = [(block, *pair_at(4 * g + i)) for i in range(4) for block in range(2)]
        work = []
        for block, at, upper in spots:
            here = pl.ds(block * BLOCK, BLOCK)
            there = pl.ds(ROWS + block * BLOCK, BLOCK)
            work.append(
                (
                    query[here, at], None,
                    jnp.concatenate([keyval[here, at], keyval[there, at]], axis=0), None,
                    jnp.concatenate([keyval[here, upper], keyval[there, upper]], axis=0),
                )
            )
        for (block, at, _), out in zip(spots, attend_pairs(work)):
            rows_a[pl.ds(block * BLOCK, BLOCK), at] = out
        return carry

    lax.fori_loop(0, 2, process_pairs, 0)
    loads[7].wait()

    def store_mesh_out(at, out):
        rows_b[:, at] = (mid[:, at].astype(F32) + out).astype(BF)

    project(rows_a, po, D, 0, store_mesh_out)
    norm_into(rows_b, 0, rows_a, 0, decode_mesh_gain)
    loads[8].wait()
    project(rows_a, dkv, 2 * D, 0, store_own)

    mine = pl.ds(0, ROWS)
    for chunk in range(4):
        here = pl.ds(chunk * BLOCK, BLOCK)
        wait_for(recv2, 32 * chunk, 32 * chunk + 32, recv_sems.at[3 + chunk])
        unpack(recv2, wide_rows, unmix, 2 * chunk, 2 * chunk + 2)

        spots = [pair_at(i) for i in range(8)]
        outs = attend_pairs(
            [
                (
                    wide_rows[here, at], query_tags[here, :],
                    keyval[mine, at], node_tag, keyval[mine, upper],
                )
                for at, upper in spots
            ]
        )
        for (at, _), out in zip(spots, outs):
            rows_a[pl.ds(0, BLOCK), at] = out
        for j in range(2):
            store_slabs(send3, 2 * chunk + j, rows_a[pl.ds(64 * j, 64), :], mix)
        send_planes(send3, recv3, 3, 7 + chunk, chunk // 2, chunk % 2 * 2, chunk % 2 * 2 + 2, -1)
    recv3[0] = send3[0]
    slot_column = jnp.sum(
        jnp.where(iota((ROWS, ROWS), 0) == iota((ROWS, ROWS), 1), d_slot, 0).astype(F32),
        axis=1,
        keepdims=True,
    )
    wait_for(send1, 0, DEVICES, send_sems.at[0])
    wait_for(lab_send, 0, DEVICES, send_sems.at[1])
    wait_for(send2, 0, DEVICES, send_sems.at[2])
    decoded = None
    for chunk in range(4):
        choose = ones_where(
            (iota((ROWS, BLOCK), 1) + chunk * BLOCK).astype(F32) == slot_column
        )
        wait_for(recv3, 32 * chunk, 32 * chunk + 32, recv_sems.at[7 + chunk])
        unpack(recv3, wide_rows, unmix, 2 * chunk, 2 * chunk + 2)
        found = matmul(choose, wide_rows[pl.ds(chunk * BLOCK, BLOCK), :])
        decoded = found if decoded is None else decoded + found
    rows_b[...] = decoded.astype(BF)
    loads[9].wait()

    def store_out(at, out):
        out_ref[:, at] = out.astype(BF)

    project(rows_b, do, D, 0, store_out)
    wait_for(send3, 0, DEVICES, send_sems.at[3])


def on_device(
    grid_state, mesh_state, encode_block, neighbour_block, decode_block,
    encode_grid_gain, encode_mesh_gain, process_gain, decode_grid_gain, decode_mesh_gain,
    encode_query, encode_keyval, encode_out, process_qkv, process_out,
    decode_query, decode_keyval, decode_out,
):
    hbm = pl.BlockSpec(memory_space=pl.ANY)
    vmem = pl.BlockSpec(memory_space=pltpu.VMEM)
    slabs = pltpu.VMEM((DEVICES, 16, 256), BF)
    rows = pltpu.VMEM((ROWS, D), BF)
    ids, gain = pltpu.VMEM((1, ROWS), jnp.int32), pltpu.VMEM((1, D), F32)
    return pl.pallas_call(
        kernel,
        out_shape=jax.ShapeDtypeStruct((ROWS, D), BF),
        in_specs=[hbm] * 18,
        out_specs=vmem,
        scratch_shapes=[
            ids, ids, pltpu.VMEM((1, 2), jnp.int32), gain, gain, gain, gain, gain,
            rows, rows,
            pltpu.VMEM((D, D), BF), pltpu.VMEM((D, 2 * D), BF), pltpu.VMEM((D, D), BF),
            pltpu.VMEM((D, 3 * D), BF), pltpu.VMEM((D, D), BF), pltpu.VMEM((D, D), BF),
            pltpu.VMEM((D, 2 * D), BF), pltpu.VMEM((D, D), BF),
            slabs, slabs, slabs, slabs, slabs, slabs,
            pltpu.VMEM((DEVICES, PAIR), F32),
            pltpu.VMEM((DEVICES, 1, PAIR), F32), pltpu.VMEM((DEVICES, 1, PAIR), F32),
            rows, rows, rows, rows,
            pltpu.VMEM((3 * ROWS, D), BF), pltpu.VMEM((SLOTS, D), BF),
            pltpu.VMEM((SLOTS, 2 * D), BF),
            pltpu.VMEM((SLOTS, PAIR), BF), pltpu.VMEM((SLOTS, PAIR), BF),
            pltpu.SemaphoreType.DMA((18,)), pltpu.SemaphoreType.DMA((4,)),
            pltpu.SemaphoreType.DMA((11,)), pltpu.SemaphoreType.DMA((8,)),
        ],
        compiler_params=pltpu.CompilerParams(
            collective_id=0, has_side_effects=True, vmem_limit_bytes=60 * 1024 * 1024
        ),
    )(
        grid_state, mesh_state, encode_block.reshape(1, -1), decode_block.reshape(1, -1),
        neighbour_block.reshape(1, -1),
        *(
            value.reshape(1, -1)
            for value in (
                encode_grid_gain, encode_mesh_gain, process_gain, decode_grid_gain, decode_mesh_gain,
            )
        ),
        encode_query, encode_keyval, encode_out, process_qkv, process_out,
        decode_query, decode_keyval, decode_out,
    )


def solution(mesh):
    rows, split = P(("gx", "gy"), None), P(("gx", "gy"))
    return jax.shard_map(
        on_device,
        mesh=mesh,
        in_specs=(rows, rows, split, split, split) + (P(),) * 13,
        out_specs=rows,
        check_vma=False,
    )
```

```python
import math

import jax
import jax.numpy as jnp
from jax import lax
from jax.experimental import pallas as pl
from jax.experimental.pallas import tpu as pltpu
from jax.sharding import PartitionSpec as P

HEADS = 16
BLOCK = 128
CAP = 4
DEVICES = 128
D = 1024
ROWS = 256
SLOTS = DEVICES * CAP
PAIR = 128
MASKED = -1e30
SCORE_SCALE = 0.125 * math.log2(math.e)
MESH = pl.DeviceIdType.MESH
BF = jnp.bfloat16
F32 = jnp.float32


def coordinates():
    gy = lax.axis_index("gy")
    return lax.axis_index("gx"), gy // 8, lax.rem(gy // 2, 4), lax.rem(gy, 2)


def each_peer(visit, core, first, last, sign):
    z, x, y, c = coordinates()
    columns = [lax.rem(x + i, 4) * 8 for i in range(4)]
    lines = [lax.rem(y + i, 4) * 2 for i in range(4)]
    side = c if core == 0 else 1 - c

    def plane(kz, start):
        gx = lax.rem(z + sign * kz + 4, 4)
        for ky in range(4):
            line = lines[sign * ky % 4] + side
            for kx in range(4):
                if kx + 4 * ky >= start:
                    visit(64 * core + 16 * kz + 4 * ky + kx, (gx, columns[sign * kx % 4] + line))

    if core == 0 and first == 0:
        plane(0, 1)
        first = 1

    def step(kz, carry):
        plane(kz, 0)
        return carry

    lax.fori_loop(first, last, step, 0)


def iota(shape, dim):
    return lax.broadcasted_iota(jnp.int32, shape, dim)


def ones_where(condition, dtype=BF):
    return jnp.where(condition, 1.0, 0.0).astype(dtype)


def matmul(a, b):
    return jnp.dot(a, b, preferred_element_type=F32)


def matmul_nt(a, b):
    return lax.dot_general(a, b, (((1,), (1,)), ((), ())), preferred_element_type=F32)


def norm_into(src, src_row, dst, dst_row, gain_ref, rows=ROWS):
    def step(i, carry):
        wide = src[pl.ds(pl.multiple_of(src_row + i * 32, 32), 32), :].astype(F32)
        scale = lax.rsqrt(jnp.mean(wide * wide, axis=-1, keepdims=True) + 1e-6)
        dst[pl.ds(pl.multiple_of(dst_row + i * 32, 32), 32), :] = (
            wide * scale * gain_ref[...]
        ).astype(BF)
        return carry

    lax.fori_loop(0, rows // 32, step, 0)


def project(a_ref, w_ref, columns, first_column, epilogue, tile=512):
    def step(n, carry):
        at = pl.multiple_of(n * tile, tile)
        out = matmul(a_ref[...], w_ref[:, pl.ds(pl.multiple_of(first_column + at, tile), tile)])
        epilogue(pl.ds(at, tile), out)
        return carry

    lax.fori_loop(0, columns // tile, step, 0, unroll=True)


def slot_plan(blocks):
    z, x, y, c = coordinates()
    owner = blocks >> 1
    k = (
        (((owner >> 3) & 3) - x & 3)
        + 4 * (((owner >> 1) & 3) - y & 3)
        + 16 * ((owner >> 5) - z & 3)
        + 64 * ((owner & 1) - c & 1)
    )
    matches = ones_where(iota((DEVICES, ROWS), 0) == k)
    earlier = ones_where(iota((ROWS, ROWS), 0) < iota((ROWS, ROWS), 1))
    counts = matmul(matches, earlier)
    rank = jnp.sum(matches.astype(F32) * counts, axis=0, keepdims=True).astype(jnp.int32)
    return matches, rank, k * CAP + rank


def label_table(matches, rank, blocks, base):
    coded = jnp.where(iota((PAIR, ROWS), 0) == rank + base, (blocks & 1) + 1, 0)
    return matmul_nt(matches, coded.astype(F32).astype(BF))


def interleave():
    m = iota((256, 256), 0)
    return ones_where(iota((256, 256), 1) == 64 * ((m >> 2) & 3) + 4 * (m >> 4) + (m & 3))


def separate():
    n = iota((256, 256), 0)
    return ones_where(iota((256, 256), 1) == 16 * ((n >> 2) & 15) + 4 * (n >> 6) + (n & 3))


def store_slabs(dst, j, rows, mix):
    tall = jnp.concatenate([rows[:, 256 * q : 256 * q + 256] for q in range(4)], axis=0)
    dst[pl.ds(16 * j, 16)] = matmul(mix, tall).astype(BF).reshape(16, 16, 256)


def load_slabs(src, j, unmix):
    tall = matmul(unmix, src[pl.ds(16 * j, 16)].reshape(256, 256)).astype(BF)
    return jnp.concatenate([tall[64 * q : 64 * q + 64] for q in range(4)], axis=1)


def pack(rows_ref, slot, dst, mix, half):
    chosen = ones_where(iota((ROWS, ROWS), 0) + ROWS * half == slot)
    rows = matmul(chosen, rows_ref[...]).astype(BF)
    for j in range(4):
        store_slabs(dst, 4 * half + j, rows[64 * j : 64 * j + 64], mix)


def unpack(src, dst, unmix, first, last):
    def step(j, carry):
        dst[pl.ds(pl.multiple_of(64 * j, 64), 64), :] = load_slabs(src, j, unmix)
        return carry

    lax.fori_loop(first, last, step, 0, unroll=True)


def attend_pairs(pairs):
    lane = iota((1, PAIR), 1)
    scores, outs = [], []
    for queries, query_tag, keys, key_tag, values in pairs:
        if key_tag is not None:
            keys = jnp.concatenate([keys, key_tag], axis=1)
        for half in range(2):
            part = queries * ones_where((lane >= 64) == (half == 1))
            if query_tag is not None:
                part = jnp.concatenate([part, query_tag], axis=1)
            scores.append(matmul_nt(part, keys))
    powers = [jnp.exp2(x - jnp.max(x, axis=-1, keepdims=True)).astype(BF) for x in scores]
    for i, (_, _, _, _, values) in enumerate(pairs):
        widened = jnp.concatenate([values, jnp.ones_like(values)], axis=1)
        halves = [matmul(powers[2 * i + half], widened) for half in range(2)]
        halves = [both[:, :PAIR] / both[:, PAIR:] for both in halves]
        outs.append(jnp.where(lane < 64, halves[0], halves[1]).astype(BF))
    return outs


def kernel(
    grid_hbm, mesh_hbm, eb_hbm, db_hbm, nb_hbm, eg_hbm, em_hbm, pg_hbm, dg_hbm, dm_hbm, eq_hbm, ekv_hbm, eo_hbm, pqkv_hbm, po_hbm, dq_hbm, dkv_hbm, do_hbm,
    out_ref,
    encode_block, decode_block, neighbour_block,
    encode_grid_gain, encode_mesh_gain, process_gain, decode_grid_gain, decode_mesh_gain,
    grid, mesh, eq, ekv, eo, pqkv, po, dq, dkv, do,
    send1, recv1, send2, recv2, send3, recv3, lab2d, lab_send, lab_recv,
    rows_a, rows_b, query, mid, cand, wide_rows, keyval, key_tags, query_tags,
    load_sems, send_sems, recv_sems, halo_sems,
):
    z, x, y, c = coordinates()
    me = lax.axis_index("gx") * 32 + lax.axis_index("gy")
    barrier = pltpu.get_barrier_semaphore()

    def greet(k, device):
        pl.semaphore_signal(barrier, inc=1, device_id=device, device_id_type=MESH)

    loads = [
        pltpu.make_async_copy(src, dst, load_sems.at[i])
        for i, (src, dst) in enumerate(
            (
                (grid_hbm, grid), (dq_hbm, dq), (mesh_hbm, mesh), (eq_hbm, eq), (ekv_hbm, ekv),
                (eo_hbm, eo), (pqkv_hbm, pqkv), (po_hbm, po), (dkv_hbm, dkv), (do_hbm, do),
            )
        )
    ]
    small = [
        pltpu.make_async_copy(src, dst, load_sems.at[10 + i])
        for i, (src, dst) in enumerate(
            (
                (eb_hbm, encode_block), (db_hbm, decode_block), (nb_hbm, neighbour_block),
                (eg_hbm, encode_grid_gain), (em_hbm, encode_mesh_gain), (pg_hbm, process_gain),
                (dg_hbm, decode_grid_gain), (dm_hbm, decode_mesh_gain),
            )
        )
    ]
    loads[0].start()
    for load in small:
        load.start()
    each_peer(greet, 0, 0, 4, 1)
    each_peer(greet, 1, 0, 4, 1)
    for load in loads[1:]:
        load.start()

    def send_planes(src, dst, sent, received, core, first, last, sign):
        def send(k, device):
            pltpu.make_async_remote_copy(
                src_ref=src.at[k], dst_ref=dst.at[k], send_sem=send_sems.at[sent],
                recv_sem=recv_sems.at[received], device_id=device, device_id_type=MESH,
            ).start()

        each_peer(send, core, first, last, sign)

    def wait_for(ref, first, last, sem):
        view = ref.at[pl.ds(max(1, first), last - max(1, first))]
        pltpu.make_async_copy(view, view, sem).wait()

    mix, unmix = interleave(), separate()
    for load in small:
        load.wait()
    e_matches, e_rank, e_slot = slot_plan(encode_block[...])
    loads[0].wait()
    norm_into(grid, 0, rows_a, 0, encode_grid_gain)
    pack(rows_a, e_slot, send1, mix, 0)
    pl.semaphore_wait(barrier, DEVICES - 1)
    send_planes(send1, recv1, 0, 0, 0, 0, 4, 1)
    d_matches, d_rank, d_slot = slot_plan(decode_block[...])
    lab2d[...] = label_table(e_matches, e_rank, encode_block[...], 0) + label_table(
        d_matches, d_rank, decode_block[...], CAP
    )

    def spread(k, carry):
        lab_send[k] = lab2d[pl.ds(k, 1), :]
        return carry

    lax.fori_loop(0, DEVICES, spread, 0, unroll=8)
    for core in range(2):
        send_planes(lab_send, lab_recv, 1, 2, core, 0, 4, 1)
    pack(rows_a, e_slot, send1, mix, 1)
    send_planes(send1, recv1, 0, 1, 1, 0, 4, 1)

    norm_into(grid, 0, rows_a, 0, decode_grid_gain)

    loads[1].wait()

    def store_query(at, out):
        rows_b[:, at] = (out * SCORE_SCALE).astype(BF)

    project(rows_a, dq, D, 0, store_query)
    pack(rows_b, d_slot, send2, mix, 0)
    for group in range(2):
        send_planes(send2, recv2, 2, 3 + group, 0, 2 * group, 2 * group + 2, 1)
    pack(rows_b, d_slot, send2, mix, 1)
    send_planes(send2, recv2, 2, 5, 1, 0, 1, 1)

    loads[2].wait()
    norm_into(mesh, 0, rows_a, 0, encode_mesh_gain)
    loads[3].wait()

    def store_mesh_query(at, out):
        query[:, at] = (out * SCORE_SCALE).astype(BF)

    project(rows_a, eq, D, 0, store_mesh_query)
    recv1[0] = send1[0]
    recv2[0] = send2[0]
    lab_recv[0] = lab_send[0]
    loads[4].wait()
    def key_values(group):
        wait_for(recv1, 64 * group, 64 * group + 64, recv_sems.at[group])
        unpack(recv1, wide_rows, unmix, 4 * group, 4 * group + 4)
        part = pl.ds(group * ROWS, ROWS)

        def store_keyval(at, out):
            keyval[part, at] = out.astype(BF)

        project(wide_rows.at[part], ekv, 2 * D, 0, store_keyval)

    key_values(0)
    wait_for(lab_recv, 0, DEVICES, recv_sems.at[2])

    def gather_labels(k, carry):
        lab2d[pl.ds(k, 1), :] = lab_recv[k]
        return carry

    lax.fori_loop(0, DEVICES, gather_labels, 0, unroll=8)
    spread_rows = matmul(
        ones_where((iota((SLOTS, DEVICES), 0) >> 2) == iota((SLOTS, DEVICES), 1)),
        lab2d[...].astype(BF),
    )
    slot_lane = iota((SLOTS, PAIR), 1)
    slot_rank = iota((SLOTS, PAIR), 0) & 3

    def slot_tags(base):
        label = jnp.sum(
            jnp.where(slot_lane == base + slot_rank, spread_rows, 0.0), axis=1, keepdims=True
        )
        other = label != (slot_lane + 1).astype(F32)
        return jnp.where(other & (slot_lane < 2), MASKED, 0.0).astype(BF)

    key_tags[...] = slot_tags(0)
    query_tags[...] = slot_tags(CAP)

    key_values(1)

    def pair_at(p):
        if isinstance(p, int):
            return pl.ds(p * PAIR, PAIR), pl.ds(D + p * PAIR, PAIR)
        return (
            pl.ds(pl.multiple_of(p * PAIR, PAIR), PAIR),
            pl.ds(pl.multiple_of(D + p * PAIR, PAIR), PAIR),
        )

    def halo(block, step, sem, to):
        there = lax.rem(me + step + DEVICES, DEVICES)
        return pltpu.make_async_remote_copy(
            src_ref=cand.at[pl.ds(ROWS + block * BLOCK, BLOCK)],
            dst_ref=cand.at[pl.ds(to + block * BLOCK, BLOCK)],
            send_sem=halo_sems.at[sem], recv_sem=halo_sems.at[sem + 1],
            device_id=(there // 32, lax.rem(there, 32)), device_id_type=MESH,
        )

    node_tag = ones_where(iota((ROWS, PAIR), 1) == (iota((ROWS, PAIR), 0) >> 7))

    def encode_pairs(g, carry):
        spots = [pair_at(4 * g + i) for i in range(4)]
        outs = attend_pairs(
            [
                (query[:, at], node_tag, keyval[:, at], key_tags[...], keyval[:, upper])
                for at, upper in spots
            ]
        )
        for (at, _), out in zip(spots, outs):
            rows_a[:, at] = out
        return carry

    lax.fori_loop(0, 2, encode_pairs, 0)
    halos = []
    loads[5].wait()
    for block in range(2):
        here = pl.ds(block * BLOCK, BLOCK)

        def store_mid(at, out):
            mid[here, at] = (mesh[here, at].astype(F32) + out).astype(BF)

        project(rows_a.at[here], eo, D, 0, store_mid)
        norm_into(mid, block * BLOCK, cand, ROWS + block * BLOCK, process_gain, BLOCK)
        for step, sem, to in ((1, 4 * block, 0), (-1, 4 * block + 2, 2 * ROWS)):
            halos.append(halo(block, step, sem, to))
            halos[-1].start()
    send_planes(send2, recv2, 2, 5, 1, 1, 2, 1)
    send_planes(send2, recv2, 2, 6, 1, 2, 4, 1)

    loads[6].wait()

    def store_process_query(at, out):
        query[:, at] = (out * SCORE_SCALE).astype(BF)

    def store_own(at, out):
        keyval[pl.ds(0, ROWS), at] = out.astype(BF)

    def store_other(at, out):
        keyval[pl.ds(ROWS, ROWS), at] = out.astype(BF)

    own = cand.at[pl.ds(ROWS, ROWS)]
    project(own, pqkv, D, 0, store_process_query)
    project(own, pqkv, 2 * D, D, store_own)
    for copy in halos:
        copy.wait()
    for block in range(2):
        target = jnp.sum(
            jnp.where(iota((1, 2), 1) == block, neighbour_block[...], 0).astype(F32),
            axis=1,
            keepdims=True,
        )
        position = target - (2 * me - 2).astype(F32) + jnp.zeros((1, PAIR), F32)
        picked = None
        for candidate in (block, block + 1, block + 3, block + 4):
            weight = jnp.concatenate([ones_where(position == candidate)] * (D // PAIR), axis=1)
            term = cand[pl.ds(candidate * BLOCK, BLOCK), :] * weight
            picked = term if picked is None else picked + term
        rows_b[pl.ds(block * BLOCK, BLOCK), :] = picked
    project(rows_b, pqkv, 2 * D, D, store_other)

    def process_pairs(g, carry):
        spots = [(block, *pair_at(4 * g + i)) for i in range(4) for block in range(2)]
        work = []
        for block, at, upper in spots:
            here = pl.ds(block * BLOCK, BLOCK)
            there = pl.ds(ROWS + block * BLOCK, BLOCK)
            work.append(
                (
                    query[here, at], None,
                    jnp.concatenate([keyval[here, at], keyval[there, at]], axis=0), None,
                    jnp.concatenate([keyval[here, upper], keyval[there, upper]], axis=0),
                )
            )
        for (block, at, _), out in zip(spots, attend_pairs(work)):
            rows_a[pl.ds(block * BLOCK, BLOCK), at] = out
        return carry

    lax.fori_loop(0, 2, process_pairs, 0)
    loads[7].wait()

    def store_mesh_out(at, out):
        rows_b[:, at] = (mid[:, at].astype(F32) + out).astype(BF)

    project(rows_a, po, D, 0, store_mesh_out)
    norm_into(rows_b, 0, rows_a, 0, decode_mesh_gain)
    loads[8].wait()
    project(rows_a, dkv, 2 * D, 0, store_own)

    mine = pl.ds(0, ROWS)
    for chunk in range(4):
        here = pl.ds(chunk * BLOCK, BLOCK)
        wait_for(recv2, 32 * chunk, 32 * chunk + 32, recv_sems.at[3 + chunk])
        unpack(recv2, wide_rows, unmix, 2 * chunk, 2 * chunk + 2)

        spots = [pair_at(i) for i in range(8)]
        outs = attend_pairs(
            [
                (
                    wide_rows[here, at], query_tags[here, :],
                    keyval[mine, at], node_tag, keyval[mine, upper],
                )
                for at, upper in spots
            ]
        )
        for (at, _), out in zip(spots, outs):
            rows_a[pl.ds(0, BLOCK), at] = out
        for j in range(2):
            store_slabs(send3, 2 * chunk + j, rows_a[pl.ds(64 * j, 64), :], mix)
        send_planes(send3, recv3, 3, 7 + chunk, chunk // 2, chunk % 2 * 2, chunk % 2 * 2 + 2, -1)
    recv3[0] = send3[0]
    slot_column = jnp.sum(
        jnp.where(iota((ROWS, ROWS), 0) == iota((ROWS, ROWS), 1), d_slot, 0).astype(F32),
        axis=1,
        keepdims=True,
    )
    wait_for(send1, 0, DEVICES, send_sems.at[0])
    wait_for(lab_send, 0, DEVICES, send_sems.at[1])
    wait_for(send2, 0, DEVICES, send_sems.at[2])
    loads[9].wait()
    update = None
    some = pl.ds(0, BLOCK)

    def store_projected(at, out):
        rows_a[some, at] = out.astype(BF)

    for chunk in range(4):
        choose = ones_where(
            (iota((ROWS, BLOCK), 1) + chunk * BLOCK).astype(F32) == slot_column
        )
        wait_for(recv3, 32 * chunk, 32 * chunk + 32, recv_sems.at[7 + chunk])
        unpack(recv3, wide_rows, unmix, 2 * chunk, 2 * chunk + 2)
        project(wide_rows.at[pl.ds(chunk * BLOCK, BLOCK)], do, D, 0, store_projected)
        found = matmul(choose, rows_a[some, :])
        update = found if update is None else update + found
    out_ref[...] = update.astype(BF)
    wait_for(send3, 0, DEVICES, send_sems.at[3])


def on_device(
    grid_state, mesh_state, encode_block, neighbour_block, decode_block,
    encode_grid_gain, encode_mesh_gain, process_gain, decode_grid_gain, decode_mesh_gain,
    encode_query, encode_keyval, encode_out, process_qkv, process_out,
    decode_query, decode_keyval, decode_out,
):
    hbm = pl.BlockSpec(memory_space=pl.ANY)
    vmem = pl.BlockSpec(memory_space=pltpu.VMEM)
    slabs = pltpu.VMEM((DEVICES, 16, 256), BF)
    rows = pltpu.VMEM((ROWS, D), BF)
    ids, gain = pltpu.VMEM((1, ROWS), jnp.int32), pltpu.VMEM((1, D), F32)
    return pl.pallas_call(
        kernel,
        out_shape=jax.ShapeDtypeStruct((ROWS, D), BF),
        in_specs=[hbm] * 18,
        out_specs=vmem,
        scratch_shapes=[
            ids, ids, pltpu.VMEM((1, 2), jnp.int32), gain, gain, gain, gain, gain,
            rows, rows,
            pltpu.VMEM((D, D), BF), pltpu.VMEM((D, 2 * D), BF), pltpu.VMEM((D, D), BF),
            pltpu.VMEM((D, 3 * D), BF), pltpu.VMEM((D, D), BF), pltpu.VMEM((D, D), BF),
            pltpu.VMEM((D, 2 * D), BF), pltpu.VMEM((D, D), BF),
            slabs, slabs, slabs, slabs, slabs, slabs,
            pltpu.VMEM((DEVICES, PAIR), F32),
            pltpu.VMEM((DEVICES, 1, PAIR), F32), pltpu.VMEM((DEVICES, 1, PAIR), F32),
            rows, rows, rows, rows,
            pltpu.VMEM((3 * ROWS, D), BF), pltpu.VMEM((SLOTS, D), BF),
            pltpu.VMEM((SLOTS, 2 * D), BF),
            pltpu.VMEM((SLOTS, PAIR), BF), pltpu.VMEM((SLOTS, PAIR), BF),
            pltpu.SemaphoreType.DMA((18,)), pltpu.SemaphoreType.DMA((4,)),
            pltpu.SemaphoreType.DMA((11,)), pltpu.SemaphoreType.DMA((8,)),
        ],
        compiler_params=pltpu.CompilerParams(
            collective_id=0, has_side_effects=True, vmem_limit_bytes=60 * 1024 * 1024
        ),
    )(
        grid_state, mesh_state, encode_block.reshape(1, -1), decode_block.reshape(1, -1),
        neighbour_block.reshape(1, -1),
        *(
            value.reshape(1, -1)
            for value in (
                encode_grid_gain, encode_mesh_gain, process_gain, decode_grid_gain, decode_mesh_gain,
            )
        ),
        encode_query, encode_keyval, encode_out, process_qkv, process_out,
        decode_query, decode_keyval, decode_out,
    )


def solution(mesh):
    rows, split = P(("gx", "gy"), None), P(("gx", "gy"))
    return jax.shard_map(
        on_device,
        mesh=mesh,
        in_specs=(rows, rows, split, split, split) + (P(),) * 13,
        out_specs=rows,
        check_vma=False,
    )
```
